32 devices in a mesh: rep: 2 (over x), data: 4 (over z), expert: 4 (over y, core).
Axes of the slice: x: 2, y: 2, z: 4, core: 2. Of those that a mesh axis runs over, the one named last changes fastest.
Arguments:
- x: bfloat16 [64, 512, 1536], P(('rep', 'expert', 'data')), parts along dimension 0
- expert_idx: int32 [64, 512, 8], P(('rep', 'expert', 'data')), parts along dimension 0
- gate: float32 [64, 512, 8], P(('rep', 'expert', 'data')), parts along dimension 0
- attn_gain: float32 [1536], replicated
- w_qkv: bfloat16 [1536, 40, 64], P(('data', 'expert'))
- w_out: bfloat16 [24, 64, 1536], P(None, None, ('data', 'expert'))
- moe_gain: float32 [1536], replicated
- w_gate: bfloat16 [40, 1536, 512], P('expert', 'data')
- w_up: bfloat16 [40, 1536, 512], P('expert', 'data')
- w_down: bfloat16 [40, 512, 1536], P('expert', None, 'data')
Outputs:
- output: bfloat16 [64, 512, 1536], P(('rep', 'expert', 'data')), parts along dimension 0
There are 2 independent parts. The reference program is written for one: setup_inputs(seed, part) draws one part's arguments, and reference() takes and returns one part's arrays. A program takes and returns all parts, laid end to end along the dimension named above; an argument that names none is the same for every part.
All inputs are finite; a program needn't handle non-finite values.
Results may differ from the reference program's by a relative error of at most 0.0150391.
Values are sent between devices in bfloat16 or wider.
A program may use at most 1 GiB of HBM per device.

```python
import jax
import jax.numpy as jnp
from jax import lax

MODEL_DIM = 1536
EXPERT_FF = 512
EXPERTS = 40
TOP_K = 8
NUM_HEADS = 24
KV_HEADS = 8
HEAD_DIM = 64
SEQ_LEN = 512
SEQS_DEV = 2
EXPERT_AXIS = 4
DATA_AXIS = 4

TOK_DEV = SEQS_DEV * SEQ_LEN
GROUP_DEVS = EXPERT_AXIS * DATA_AXIS
CAPACITY = 8 * ((5 * TOP_K * TOK_DEV + 32 * EXPERTS - 1) // (32 * EXPERTS))
QKV_HEADS = NUM_HEADS + 2 * KV_HEADS
GROUP_LEN = NUM_HEADS // KV_HEADS
NORM_EPS = 1e-6
ROPE_BASE = 10000.0


def draw_routing(key):
    noise_key, hot_key, perm_key = jax.random.split(key, 3)
    noise = jax.random.randint(noise_key, (GROUP_DEVS, TOK_DEV, EXPERTS), 0, 1 << 20)
    hot_ids = jax.random.randint(hot_key, (GROUP_DEVS,), 0, EXPERTS)
    perm_keys = jax.random.split(perm_key, GROUP_DEVS)
    ranks = jax.vmap(lambda one_key: jax.random.permutation(one_key, TOK_DEV))(perm_keys)
    flagged = ranks < TOK_DEV // 2
    is_hot = jnp.arange(EXPERTS)[None, None, :] == hot_ids[:, None, None]
    score = (noise + jnp.where(flagged[:, :, None] & is_hot, 1 << 21, 0)) * EXPERTS + jnp.arange(EXPERTS)[None, None, :]
    chosen = lax.top_k(score, TOP_K)[1]
    return chosen.astype(jnp.int32).reshape(GROUP_DEVS * SEQS_DEV, SEQ_LEN, TOP_K)


def setup_inputs(seed: int = 0, part: int = 0) -> dict:
    base_key = jax.random.key(seed)
    part_key = jax.random.fold_in(base_key, part)
    x_key, route_key, gate_key = jax.random.split(part_key, 3)
    weight_keys = jax.random.split(jax.random.key(seed + 1), 7)
    num_seqs = GROUP_DEVS * SEQS_DEV
    x = jax.random.normal(x_key, (num_seqs, SEQ_LEN, MODEL_DIM), jnp.float32).astype(jnp.bfloat16)
    expert_idx = draw_routing(route_key)
    gate = jax.random.uniform(gate_key, (num_seqs, SEQ_LEN, TOP_K), jnp.float32, 0.4, 1.6) * TOP_K ** -0.5
    attn_gain = jax.random.uniform(weight_keys[0], (MODEL_DIM,), jnp.float32, 0.5, 1.5)
    w_qkv = (jax.random.normal(weight_keys[1], (MODEL_DIM, QKV_HEADS, HEAD_DIM), jnp.float32) * (1.5 * MODEL_DIM ** -0.5)).astype(jnp.bfloat16)
    w_out = (jax.random.normal(weight_keys[2], (NUM_HEADS, HEAD_DIM, MODEL_DIM), jnp.float32) * (NUM_HEADS * HEAD_DIM) ** -0.5).astype(jnp.bfloat16)
    moe_gain = jax.random.uniform(weight_keys[3], (MODEL_DIM,), jnp.float32, 0.5, 1.5)
    w_gate = (jax.random.normal(weight_keys[4], (EXPERTS, MODEL_DIM, EXPERT_FF), jnp.float32) * MODEL_DIM ** -0.5).astype(jnp.bfloat16)
    w_up = (jax.random.normal(weight_keys[5], (EXPERTS, MODEL_DIM, EXPERT_FF), jnp.float32) * MODEL_DIM ** -0.5).astype(jnp.bfloat16)
    w_down = (jax.random.normal(weight_keys[6], (EXPERTS, EXPERT_FF, MODEL_DIM), jnp.float32) * (2.0 * EXPERT_FF ** -0.5)).astype(jnp.bfloat16)
    return {'x': x, 'expert_idx': expert_idx, 'gate': gate, 'attn_gain': attn_gain, 'w_qkv': w_qkv, 'w_out': w_out, 'moe_gain': moe_gain, 'w_gate': w_gate, 'w_up': w_up, 'w_down': w_down}


def rms_scale(tok_rows, gain):
    rows_f32 = tok_rows.astype(jnp.float32)
    inv_rms = lax.rsqrt(jnp.mean(rows_f32 * rows_f32, axis=-1, keepdims=True) + NORM_EPS)
    return (rows_f32 * inv_rms * gain).astype(jnp.bfloat16)


def apply_rope(head_vals):
    half_dim = HEAD_DIM // 2
    inv_freq = ROPE_BASE ** (-jnp.arange(half_dim, dtype=jnp.float32) * 2.0 / HEAD_DIM)
    angles = jnp.arange(SEQ_LEN, dtype=jnp.float32)[:, None] * inv_freq[None, :]
    cos_b = jnp.cos(angles)[:, None, :]
    sin_b = jnp.sin(angles)[:, None, :]
    vals_f32 = head_vals.astype(jnp.float32)
    low_half = vals_f32[..., :half_dim]
    high_half = vals_f32[..., half_dim:]
    return jnp.concatenate([low_half * cos_b - high_half * sin_b, high_half * cos_b + low_half * sin_b], axis=-1).astype(jnp.bfloat16)


def attend_one(seq_x, attn_gain, w_qkv, w_out):
    normed = rms_scale(seq_x, attn_gain)
    qkv_all = jnp.dot(normed, w_qkv.reshape(MODEL_DIM, QKV_HEADS * HEAD_DIM), preferred_element_type=jnp.float32).astype(jnp.bfloat16).reshape(SEQ_LEN, QKV_HEADS, HEAD_DIM)
    queries = apply_rope(qkv_all[:, :NUM_HEADS]).reshape(SEQ_LEN, KV_HEADS, GROUP_LEN, HEAD_DIM)
    keys_rot = apply_rope(qkv_all[:, NUM_HEADS:NUM_HEADS + KV_HEADS])
    values = qkv_all[:, NUM_HEADS + KV_HEADS:]
    scores = jnp.einsum('lkgd,mkd->kglm', queries.astype(jnp.float32), keys_rot.astype(jnp.float32)) * (HEAD_DIM ** -0.5)
    causal = jnp.arange(SEQ_LEN)[:, None] >= jnp.arange(SEQ_LEN)[None, :]
    attn_probs = jax.nn.softmax(jnp.where(causal, scores, -1e30), axis=-1).astype(jnp.bfloat16)
    mixed = jnp.einsum('kglm,mkd->lkgd', attn_probs.astype(jnp.float32), values.astype(jnp.float32)).astype(jnp.bfloat16)
    attn_proj = jnp.dot(mixed.reshape(SEQ_LEN, NUM_HEADS * HEAD_DIM), w_out.reshape(NUM_HEADS * HEAD_DIM, MODEL_DIM), preferred_element_type=jnp.float32)
    return (seq_x.astype(jnp.float32) + attn_proj).astype(jnp.bfloat16)


def dispatch_target(flat_ids):
    onehot = (flat_ids[:, None] == jnp.arange(EXPERTS)[None, :]).astype(jnp.int32)
    earlier = jnp.cumsum(onehot, axis=0) - onehot
    slot_pos = jnp.sum(earlier * onehot, axis=1)
    return jnp.where(slot_pos < CAPACITY, flat_ids * CAPACITY + slot_pos, EXPERTS * CAPACITY)


def run_expert(operands):
    tok_rows, gate_w, up_w, down_w = operands
    rows_f32 = tok_rows.astype(jnp.float32)
    act_gate = jnp.dot(rows_f32, gate_w.astype(jnp.float32))
    act_up = jnp.dot(rows_f32, up_w.astype(jnp.float32))
    mid_act = (jax.nn.silu(act_gate) * act_up).astype(jnp.bfloat16)
    return jnp.dot(mid_act.astype(jnp.float32), down_w.astype(jnp.float32)).astype(jnp.bfloat16)


def reference(x, expert_idx, gate, attn_gain, w_qkv, w_out, moe_gain, w_gate, w_up, w_down):
    hidden = lax.map(lambda seq_x: attend_one(seq_x, attn_gain, w_qkv, w_out), x)
    hid_dev = hidden.reshape(GROUP_DEVS, TOK_DEV, MODEL_DIM)
    ids_dev = expert_idx.reshape(GROUP_DEVS, TOK_DEV * TOP_K)
    gate_dev = gate.reshape(GROUP_DEVS, TOK_DEV, TOP_K)

    def build_buffer(operands):
        hid_rows, flat_ids = operands
        normed = rms_scale(hid_rows, moe_gain)
        target_rows = dispatch_target(flat_ids)
        filled = jnp.zeros((EXPERTS * CAPACITY + 1, MODEL_DIM), jnp.bfloat16).at[target_rows].set(jnp.repeat(normed, TOP_K, axis=0))
        return filled[:EXPERTS * CAPACITY].reshape(EXPERTS, CAPACITY, MODEL_DIM), target_rows

    buffers, target_all = lax.map(build_buffer, (hid_dev, ids_dev))
    by_expert = jnp.transpose(buffers, (1, 0, 2, 3)).reshape(EXPERTS, GROUP_DEVS * CAPACITY, MODEL_DIM)
    expert_out = lax.map(run_expert, (by_expert, w_gate, w_up, w_down))
    out_dev = jnp.transpose(expert_out.reshape(EXPERTS, GROUP_DEVS, CAPACITY, MODEL_DIM), (1, 0, 2, 3)).reshape(GROUP_DEVS, EXPERTS * CAPACITY, MODEL_DIM)

    def combine(operands):
        hid_rows, out_rows, target_rows, gate_rows = operands
        padded = jnp.concatenate([out_rows, jnp.zeros((1, MODEL_DIM), jnp.bfloat16)], axis=0)
        picked = jnp.take(padded, target_rows, axis=0).reshape(TOK_DEV, TOP_K, MODEL_DIM).astype(jnp.float32)
        total = hid_rows.astype(jnp.float32) + jnp.sum(picked * gate_rows[:, :, None], axis=1)
        return total.astype(jnp.bfloat16)

    result = lax.map(combine, (hid_dev, out_dev, target_all, gate_dev))
    return result.reshape(GROUP_DEVS * SEQS_DEV, SEQ_LEN, MODEL_DIM)
```

```python
import functools

import jax
import jax.numpy as jnp
from jax import lax
from jax.experimental import pallas as pl
from jax.experimental.pallas import tpu as pltpu
from jax.sharding import PartitionSpec as P


NORM_EPS = 1e-6
ROPE_BASE = 10000.0
F32 = jnp.float32
BF16 = jnp.bfloat16
VMEM_LIMIT = 58 * 1024 * 1024


def qkv_kernel(rope_cols, half_dim, x_ref, gain_ref, w_ref, cos_ref, sin_ref, o_ref):
    rows_f32 = x_ref[...].astype(F32)
    inv_rms = lax.rsqrt(jnp.mean(rows_f32 * rows_f32, axis=-1, keepdims=True) + NORM_EPS)
    normed = (rows_f32 * inv_rms * gain_ref[...]).astype(BF16)
    lanes = 128
    low = lax.broadcasted_iota(jnp.int32, cos_ref.shape, 1) % (2 * half_dim) < half_dim
    for c in range(0, w_ref.shape[1], 2 * lanes):
        part = jnp.dot(normed, w_ref[:, c:c + 2 * lanes], preferred_element_type=F32).astype(BF16)
        if c >= rope_cols:
            o_ref[:, c:c + 2 * lanes] = part
            continue
        for b in range(0, 2 * lanes, lanes):
            vals = part[:, b:b + lanes].astype(F32)
            other = jnp.where(low, pltpu.roll(vals, lanes - half_dim, 1), pltpu.roll(vals, half_dim, 1))
            o_ref[:, c + b:c + b + lanes] = (vals * cos_ref[...] + other * sin_ref[...]).astype(BF16)


def qkv_project(x, gain, w_qkv, cos_t, sin_t, rope_cols, half_dim):
    toks, width = x.shape
    seq_len = cos_t.shape[0]
    cols = w_qkv.shape[1]
    fixed = lambda shape: pl.BlockSpec(shape, lambda i: (0, 0))
    return pl.pallas_call(
        functools.partial(qkv_kernel, rope_cols, half_dim), name="k_qkv", grid=(toks // seq_len,),
        in_specs=[pl.BlockSpec((seq_len, width), lambda i: (i, 0)), fixed((1, width)), fixed(w_qkv.shape), fixed(cos_t.shape), fixed(sin_t.shape)],
        out_specs=pl.BlockSpec((seq_len, cols), lambda i: (i, 0)),
        out_shape=jax.ShapeDtypeStruct((toks, cols), BF16),
        cost_estimate=pl.CostEstimate(flops=2 * toks * width * cols, bytes_accessed=2 * (toks * width + width * cols + toks * cols), transcendentals=0),
        compiler_params=pltpu.CompilerParams(vmem_limit_bytes=VMEM_LIMIT),
    )(x, gain, w_qkv, cos_t, sin_t)


def attend_kernel(group_len, head_dim, q_ref, k_ref, v_ref, o_ref):
    seq_len = q_ref.shape[0]
    tile = 256
    scale = head_dim ** -0.5 * 1.4426950408889634
    for kh in range(k_ref.shape[1] // head_dim):
        keys = k_ref[:, kh * head_dim:(kh + 1) * head_dim]
        vals = v_ref[:, kh * head_dim:(kh + 1) * head_dim]
        for g in range(group_len):
            c = (kh * group_len + g) * head_dim
            for r in range(0, seq_len, tile):
                seen = r + tile
                scores = lax.dot_general(q_ref[r:seen, c:c + head_dim], keys[:seen], (((1,), (1,)), ((), ())), preferred_element_type=F32)
                causal = lax.broadcasted_iota(jnp.int32, scores.shape, 0) + r >= lax.broadcasted_iota(jnp.int32, scores.shape, 1)
                scores = jnp.where(causal, scores, -1e30)
                top = jnp.max(scores, axis=-1, keepdims=True)
                weights = jnp.exp2((scores - top) * scale)
                probs = (weights * (1.0 / jnp.sum(weights, axis=-1, keepdims=True))).astype(BF16)
                o_ref[r:seen, c:c + head_dim] = jnp.dot(probs, vals[:seen], preferred_element_type=F32).astype(BF16)


def attend(qkv, seq_len, num_heads, kv_heads, head_dim):
    toks = qkv.shape[0]
    group_len = num_heads // kv_heads
    pair = 128 // head_dim
    qcols = pair * group_len * head_dim
    kcol0 = num_heads * head_dim // 128
    vcol0 = (num_heads + kv_heads) * head_dim // 128
    return pl.pallas_call(
        functools.partial(attend_kernel, group_len, head_dim), name="k_attn", grid=(toks // seq_len, kv_heads // pair),
        in_specs=[pl.BlockSpec((seq_len, qcols), lambda s, j: (s, j)), pl.BlockSpec((seq_len, 128), lambda s, j: (s, kcol0 + j)),
                  pl.BlockSpec((seq_len, 128), lambda s, j: (s, vcol0 + j))],
        out_specs=pl.BlockSpec((seq_len, qcols), lambda s, j: (s, j)),
        out_shape=jax.ShapeDtypeStruct((toks, num_heads * head_dim), BF16),
        cost_estimate=pl.CostEstimate(flops=16 * toks * seq_len * num_heads * head_dim, bytes_accessed=2 * toks * (qkv.shape[1] + num_heads * head_dim), transcendentals=toks * seq_len * num_heads),
        compiler_params=pltpu.CompilerParams(vmem_limit_bytes=VMEM_LIMIT),
    )(qkv, qkv, qkv)


def project_kernel(a_ref, w_ref, x_ref, gain_ref, h_ref, z_ref):
    proj = lax.dot_general(a_ref[...], w_ref[...], (((1,), (1,)), ((), ())), preferred_element_type=F32)
    hidden = (x_ref[...].astype(F32) + proj).astype(BF16)
    h_ref[...] = hidden
    rows_f32 = hidden.astype(F32)
    inv_rms = lax.rsqrt(jnp.mean(rows_f32 * rows_f32, axis=-1, keepdims=True) + NORM_EPS)
    z_ref[...] = (rows_f32 * inv_rms * gain_ref[...]).astype(BF16)


def project(mixed, w_out_t, x, gain):
    toks, width = x.shape
    tile = 256
    row = lambda n: pl.BlockSpec((tile, n), lambda i: (i, 0))
    fixed = lambda shape: pl.BlockSpec(shape, lambda i: (0, 0))
    return pl.pallas_call(
        project_kernel, name="k_out", grid=(toks // tile,),
        in_specs=[row(mixed.shape[1]), fixed(w_out_t.shape), row(width), fixed((1, width))],
        out_specs=[row(width)] * 2,
        out_shape=[jax.ShapeDtypeStruct((toks, width), BF16)] * 2,
        cost_estimate=pl.CostEstimate(flops=2 * toks * width * mixed.shape[1], bytes_accessed=2 * (4 * toks * width + width * width), transcendentals=0),
        compiler_params=pltpu.CompilerParams(vmem_limit_bytes=VMEM_LIMIT),
    )(mixed, w_out_t, x, gain)


def attention_block(seqs, attn_gain, w_qkv, w_out_t, num_heads, kv_heads, head_dim, moe_gain):
    num_seqs, seq_len, width = seqs.shape
    half_dim = head_dim // 2
    inv_freq = ROPE_BASE ** (-jnp.arange(half_dim, dtype=F32) * 2.0 / head_dim)
    angles = jnp.arange(seq_len, dtype=F32)[:, None] * inv_freq[None, :]
    cos_t, sin_t = jnp.cos(angles), jnp.sin(angles)
    cos_t = jnp.concatenate([cos_t] * (128 // half_dim), axis=1)
    sin_t = jnp.concatenate([-sin_t, sin_t] * (64 // half_dim), axis=1)
    x = seqs.reshape(num_seqs * seq_len, width)
    qkv = qkv_project(x, attn_gain.reshape(1, width), w_qkv, cos_t, sin_t, (num_heads + kv_heads) * head_dim, half_dim)
    mixed = attend(qkv, seq_len, num_heads, kv_heads, head_dim)
    return project(mixed, w_out_t, x, moe_gain.reshape(1, width))


def dispatch_kernel(half, cap, rank_ref, rows_ref, buf_ref, out_ref, hot_ref):
    del buf_ref
    step = pl.program_id(0)
    toks, width = rows_ref.shape
    slots = lax.broadcasted_iota(jnp.int32, (cap, toks), 0).astype(F32)
    for i in range(half):
        ranks = rank_ref[pl.ds(step * half + i, 1), :]
        hot_ref[i * cap:(i + 1) * cap, :] = jnp.where(slots == ranks, 1.0, 0.0).astype(BF16)
    for c in range(0, width, 512):
        part = jnp.dot(hot_ref[...], rows_ref[:, c:c + 512], preferred_element_type=F32)
        out_ref[:, 0, :, c:c + 512] = part.astype(BF16).reshape(half, cap, 512)


def dispatch(rank_rows, rows, buf, slot, experts, cap, sources):
    toks, width = rows.shape
    half = experts // 2
    alias = {} if buf is None else {2: 0}
    args = (rank_rows, rows) + (() if buf is None else (buf,))
    body = functools.partial(dispatch_kernel, half, cap)
    if buf is None:
        def body(rank_ref, rows_ref, out_ref, hot_ref):
            dispatch_kernel(half, cap, rank_ref, rows_ref, None, out_ref, hot_ref)
    in_specs = [pl.BlockSpec(rank_rows.shape, lambda g: (0, 0)), pl.BlockSpec((toks, width), lambda g: (0, 0))]
    if buf is not None:
        in_specs.append(pl.BlockSpec(memory_space=pl.ANY))
    return pl.pallas_call(
        body, grid=(2,),
        out_shape=jax.ShapeDtypeStruct((experts, sources, cap, width), BF16),
        in_specs=in_specs,
        out_specs=pl.BlockSpec((half, 1, cap, width), lambda g: (g, slot, 0, 0)),
        scratch_shapes=[pltpu.VMEM((half * cap, toks), BF16)],
        input_output_aliases=alias,
        cost_estimate=pl.CostEstimate(flops=2 * experts * cap * toks * width, bytes_accessed=2 * (toks + experts * cap) * width, transcendentals=0),
        compiler_params=pltpu.CompilerParams(vmem_limit_bytes=VMEM_LIMIT),
    )(*args)


def gate_up_kernel(steps, s_ref, x_ref, *refs):
    g_refs, u_refs = refs[:steps], refs[steps:2 * steps]
    m_ref, wg_ref, wu_ref = refs[2 * steps:]
    d = s_ref[1]
    depth = g_refs[0].shape[1]
    for t in range(steps):
        rows = pl.ds(pl.multiple_of(lax.rem(d + steps - t, steps) * depth, depth), depth)
        wg_ref[rows, :] = g_refs[t][0]
        wu_ref[rows, :] = u_refs[t][0]
    x = x_ref[0]
    act = jnp.dot(x, wg_ref[...], preferred_element_type=F32)
    up = jnp.dot(x, wu_ref[...], preferred_element_type=F32)
    m_ref[0] = (act * jax.nn.sigmoid(act) * up).astype(BF16)


def gate_up(scal, x, which, gates, ups):
    half, depth, ff = gates[1].shape
    steps = len(gates)
    _, rows, width = x.shape
    own = pl.BlockSpec((1, depth, ff), lambda i, s: (s[0] + i, 0, 0))
    piece = pl.BlockSpec((1, depth, ff), lambda i, s: (i, 0, 0))
    return pl.pallas_call(
        functools.partial(gate_up_kernel, steps),
        grid_spec=pltpu.PrefetchScalarGridSpec(
            num_scalar_prefetch=1, grid=(half,),
            in_specs=[pl.BlockSpec((1, rows, width), lambda i, s: (which * half + i, 0, 0))] + ([own] + [piece] * (steps - 1)) * 2,
            out_specs=pl.BlockSpec((1, rows, ff), lambda i, s: (i, 0, 0)),
            scratch_shapes=[pltpu.VMEM((width, ff), BF16)] * 2),
        out_shape=jax.ShapeDtypeStruct((half, rows, ff), BF16),
        cost_estimate=pl.CostEstimate(flops=4 * half * rows * width * ff, bytes_accessed=2 * half * (rows * width + 2 * width * ff), transcendentals=0),
        compiler_params=pltpu.CompilerParams(vmem_limit_bytes=VMEM_LIMIT),
    )(scal, x, *gates, *ups)


def combine_kernel(half, adds, s_ref, table_ref, ma_ref, mb_ref, wa_ref, wb_ref, *refs):
    del s_ref
    add_refs, (o0_ref, o1_ref, acc_ref) = refs[:adds], refs[adds:]
    g = pl.program_id(0)
    toks, cap = table_ref.shape[1], ma_ref.shape[1]
    table = table_ref[0]
    slots = lax.broadcasted_iota(jnp.int32, (toks, cap), 1).astype(F32)
    for e in range(2 * half):
        m_ref, w_ref, i = (ma_ref, wa_ref, e) if e < half else (mb_ref, wb_ref, e - half)
        o = jnp.dot(m_ref[i], w_ref[i], preferred_element_type=F32).astype(BF16)
        hot = jnp.where(slots == table[:, e:e + 1], 1.0, 0.0).astype(BF16)
        picked = jnp.dot(hot, o, preferred_element_type=F32) * table[:, 2 * half + e:2 * half + e + 1]
        if e == 0:
            acc_ref[...] = picked
        else:
            acc_ref[...] += picked

    @pl.when(g == 0)
    def _():
        o0_ref[...] = acc_ref[...] + add_refs[0][...] if adds else acc_ref[...]

    @pl.when(g == 1)
    def _():
        o1_ref[...] = acc_ref[...] + add_refs[1][...] if adds else acc_ref[...]


def combine(scal, table, first, stride, mids, downs, adds):
    sources, toks, lanes = table.shape
    half, rows, ff = mids[0].shape
    cap = rows // sources
    cols = downs[0].shape[2]
    src = lambda g: first + stride * g
    whole = pl.BlockSpec((toks, cols), lambda g, s: (0, 0))
    return pl.pallas_call(
        functools.partial(combine_kernel, half, len(adds)),
        grid_spec=pltpu.PrefetchScalarGridSpec(
            num_scalar_prefetch=1, grid=(2,),
            in_specs=[pl.BlockSpec((1, toks, lanes), lambda g, s: (src(g), 0, 0)),
                      pl.BlockSpec((half, cap, ff), lambda g, s: (0, src(g), 0)),
                      pl.BlockSpec((half, cap, ff), lambda g, s: (0, src(g), 0)),
                      pl.BlockSpec((half, ff, cols), lambda g, s: (s[0], 0, 0)),
                      pl.BlockSpec((half, ff, cols), lambda g, s: (s[1], 0, 0))] + [whole] * len(adds),
            out_specs=[whole, whole],
            scratch_shapes=[pltpu.VMEM((toks, cols), F32)]),
        out_shape=[jax.ShapeDtypeStruct((toks, cols), F32)] * 2,
        cost_estimate=pl.CostEstimate(flops=2 * 2 * half * 2 * cap * cols * (ff + toks), bytes_accessed=2 * 2 * half * (ff * cols + 2 * cap * ff) + 8 * toks * cols * (1 + len(adds) // 2), transcendentals=0),
        compiler_params=pltpu.CompilerParams(vmem_limit_bytes=VMEM_LIMIT),
    )(scal, table, *mids, *downs, *adds)


def finish_kernel(steps, s_ref, h_ref, *refs):
    own, far, y_ref = refs[:steps], refs[steps:2 * steps], refs[2 * steps]
    cols = own[0].shape[1]
    for t in range(steps):
        at = pl.ds(pl.multiple_of(lax.rem(s_ref[0] + steps - t, steps) * cols, 128), cols)
        y_ref[:, at] = (h_ref[:, at].astype(F32) + (own[t][...] + far[t][...])).astype(BF16)


def finish(scal, hidden, own, far):
    toks, width = hidden.shape
    cols = own[0].shape[1]
    tile = 256
    wide = pl.BlockSpec((tile, width), lambda i, s: (i, 0))
    part = pl.BlockSpec((tile, cols), lambda i, s: (i, 0))
    return pl.pallas_call(
        functools.partial(finish_kernel, len(own)), name="finish",
        grid_spec=pltpu.PrefetchScalarGridSpec(
            num_scalar_prefetch=1, grid=(toks // tile,),
            in_specs=[wide] + [part] * (2 * len(own)), out_specs=wide),
        out_shape=jax.ShapeDtypeStruct((toks, width), BF16),
        cost_estimate=pl.CostEstimate(flops=2 * toks * width, bytes_accessed=12 * toks * width, transcendentals=0),
        compiler_params=pltpu.CompilerParams(vmem_limit_bytes=VMEM_LIMIT),
    )(scal, hidden, *own, *far)


def solution(mesh):
    sources = mesh.shape['expert']
    steps = mesh.shape['data']
    tok_spec = P(('rep', 'expert', 'data'), None, None)
    group_axes = ('data', 'expert')
    ring = [(i, (i + 1) % steps) for i in range(steps)]
    flip = [[(i, i ^ k) for i in range(sources)] for k in range(sources)]
    swap = [(0, 1), (1, 0)]

    def local_step(x_loc, idx_loc, gate_loc, attn_gain, qkv_part, out_part, moe_gain, gate_part, up_part, down_part):
        rep, data, expert = (lax.axis_index(a) for a in ('rep', 'data', 'expert'))
        num_seqs, seq_len, width = x_loc.shape
        toks = num_seqs * seq_len
        top_k = idx_loc.shape[-1]
        experts = gate_part.shape[0]
        half = experts // 2
        cap = 8 * ((5 * top_k * toks + 32 * experts * sources - 1) // (32 * experts * sources))
        heads_all, head_dim = qkv_part.shape[1:]
        num_heads = out_part.shape[0]

        def pieces(w):
            mine = lax.dynamic_slice_in_dim(w, rep * half, half, 0)
            near, far = [], []
            for _ in range(1, steps):
                mine = lax.ppermute(mine, 'data', ring)
                near.append(mine)
                far.append(lax.ppermute(mine, 'rep', swap))
            return near, far

        w_qkv = lax.all_gather(qkv_part.reshape(qkv_part.shape[0], heads_all * head_dim), group_axes, axis=0, tiled=True)
        w_out_t = lax.all_gather(out_part.reshape(num_heads * head_dim, -1).T, group_axes, axis=0, tiled=True)
        g_near, g_far = pieces(gate_part)
        u_near, u_far = pieces(up_part)
        d_near, d_far = pieces(down_part)

        idx_t = idx_loc.reshape(toks, top_k).T
        gate_t = gate_loc.reshape(toks, top_k).T
        idx_all = jnp.stack([idx_t] + [lax.ppermute(idx_t, 'expert', flip[k]) for k in range(1, sources)])
        gate_all = jnp.stack([gate_t] + [lax.ppermute(gate_t, 'expert', flip[k]) for k in range(1, sources)])
        order = lax.iota(jnp.int32, experts)
        local_ids = expert * experts + (order // half + rep) % 2 * half + order % half
        match = idx_all[:, :, None, :] == local_ids[None, None, :, None]
        taken = jnp.any(match, axis=1)
        weight = jnp.sum(jnp.where(match, gate_all[:, :, None, :], 0.0), axis=1)
        before = (lax.broadcasted_iota(jnp.int32, (toks, toks), 0) < lax.broadcasted_iota(jnp.int32, (toks, toks), 1)).astype(BF16)
        rank = jnp.dot(taken.reshape(sources * experts, toks).astype(BF16), before, preferred_element_type=F32).reshape(sources, experts, toks)
        rank = jnp.where(taken & (rank < cap), rank, -1.0)
        rank_rows = jnp.pad(rank, ((0, 0), (0, 16 - experts), (0, 0)), constant_values=-1.0)
        table = jnp.pad(jnp.concatenate([rank, weight], axis=1), ((0, 0), (0, 128 - 2 * experts), (0, 0))).transpose(0, 2, 1)

        attn_gain, rank_rows, table = lax.optimization_barrier((attn_gain, rank_rows, table))
        hidden, normed = attention_block(x_loc, attn_gain, w_qkv, w_out_t, num_heads, (heads_all - num_heads) // 2, head_dim, moe_gain)
        z_y = lax.ppermute(normed, 'expert', flip[2])
        z_c = lax.ppermute(normed, 'expert', flip[1])
        z_yc = lax.ppermute(z_y, 'expert', flip[1])
        buf = None
        for k, rows in enumerate((normed, z_c, z_y, z_yc)):
            buf = dispatch(rank_rows[k], rows, buf, k, experts, cap, sources)
        x_all = buf.reshape(experts, sources * cap, width)

        scal = jnp.stack([rep * half, data]).astype(jnp.int32)
        scal_far = jnp.stack([(1 - rep) * half, data]).astype(jnp.int32)
        mid_near = gate_up(scal, x_all, 0, [gate_part] + g_near, [up_part] + u_near)
        mid_far = gate_up(scal_far, x_all, 1, [gate_part] + g_far, [up_part] + u_far)
        mids = (mid_near, mid_far)

        own_s = jnp.stack([rep, 1 - rep]).astype(jnp.int32)
        zero_s = jnp.zeros((2,), jnp.int32)
        own, far = [], []
        for t in range(steps):
            downs = (down_part, down_part) if t == 0 else (d_near[t - 1], d_far[t - 1])
            s = own_s if t == 0 else zero_s
            p1, p3 = combine(s, table, 1, 2, mids, downs, ())
            r1, r3 = lax.ppermute(p1, 'expert', flip[1]), lax.ppermute(p3, 'expert', flip[1])
            a0, a2 = combine(s, table, 0, 2, mids, downs, (r1, r3))
            own.append(a0)
            far.append(lax.ppermute(a2, 'expert', flip[2]))
        y = finish(data.reshape(1).astype(jnp.int32), hidden, own, far)
        return y.reshape(num_seqs, seq_len, width)

    in_specs = (tok_spec, tok_spec, tok_spec, P(None), P(group_axes, None, None), P(None, None, group_axes), P(None), P('expert', 'data', None), P('expert', 'data', None), P('expert', None, 'data'))

    return jax.shard_map(local_step, mesh=mesh, in_specs=in_specs, out_specs=tok_spec, check_vma=False)
```

```python
import functools

import jax
import jax.numpy as jnp
from jax import lax
from jax.experimental import pallas as pl
from jax.experimental.pallas import tpu as pltpu
from jax.sharding import PartitionSpec as P


NORM_EPS = 1e-6
ROPE_BASE = 10000.0
F32 = jnp.float32
BF16 = jnp.bfloat16
VMEM_LIMIT = 58 * 1024 * 1024


def gather_kernel(names, sizes, q_ref, o_ref, g_ref, wq_ref, wo_ref, g1_ref, send, recv, extra, local):
    rep, data, expert = (lax.axis_index(n) for n in names)
    steps, sources = sizes
    after = lax.rem(data + 1, steps)
    across = lax.rem(expert + 2, sources)
    mate = expert + 1 - 2 * lax.rem(expert, 2)
    pairs = ((q_ref, wq_ref), (o_ref, wo_ref))
    share = q_ref.shape[0]
    half = share // 2
    right, twin, far, peer = {names[1]: after}, {names[0]: 1 - rep}, {names[2]: across}, {names[2]: mate}

    def block(w, t, e, h):
        d = lax.rem(data + steps - t, steps)
        return pairs[w][1].at[pl.ds(pl.multiple_of((d * sources + e) * share + h * half, 16), half), :]

    def whole(w, e):
        return pairs[w][1].at[pl.ds(pl.multiple_of((data * sources + e) * share, 16), share), :]

    def copy(w, j, src, dst, dev):
        return pltpu.make_async_remote_copy(src_ref=src, dst_ref=dst, send_sem=send.at[w, j], recv_sem=recv.at[w, j], device_id=dev, device_id_type=pl.DeviceIdType.MESH)

    jobs = {}
    keep = []
    for w, (own, full) in enumerate(pairs):
        mine = own.at[pl.ds(pl.multiple_of(rep * half, 16), half), :]
        keep.append(pltpu.make_async_copy(own, whole(w, expert), local.at[w]))
        jobs[w, 6] = copy(w, 6, own, whole(w, expert), far)
        jobs[w, 13] = copy(w, 13, own, whole(w, expert), peer)
        jobs[w, 20] = copy(w, 20, whole(w, across), whole(w, across), peer)
        for t in range(1, steps):
            i = t - 1
            z_src = mine if t == 1 else block(w, i, expert, rep)
            jobs[w, i] = copy(w, i, z_src, block(w, i, expert, rep), right)
            near, other = block(w, t, expert, rep), block(w, t, expert, 1 - rep)
            y_near, y_other = block(w, t, across, rep), block(w, t, across, 1 - rep)
            jobs[w, 3 + i] = copy(w, 3 + i, near, near, twin)
            jobs[w, 7 + i] = copy(w, 7 + i, near, near, far)
            jobs[w, 10 + i] = copy(w, 10 + i, y_near, y_near, twin)
            for j, b in ((14, near), (17, other), (21, y_near), (24, y_other)):
                jobs[w, j + i] = copy(w, j + i, b, b, peer)
    experts = g1_ref.shape[0]
    big = pltpu.make_async_remote_copy(src_ref=g_ref.at[pl.ds(rep * experts, experts)], dst_ref=g1_ref, send_sem=extra.at[0], recv_sem=extra.at[1],
                                       device_id=right, device_id_type=pl.DeviceIdType.MESH)

    def pass_on(arrived, *then):
        for w in range(2):
            jobs[w, arrived].wait_recv()
            for j in then:
                jobs[w, j].start()

    for w in range(2):
        for j in (0, 6, 13):
            jobs[w, j].start()
        keep[w].start()
    for i in range(3):
        pass_on(i, *(((i + 1,) if i < 2 else ()) + (3 + i, 7 + i, 14 + i)))
        if i == 2:
            big.start()
        if i == 0:
            pass_on(6, 20)
        else:
            pass_on(7 + i - 1, 10 + i - 1, 21 + i - 1)
            pass_on(3 + i - 1, 17 + i - 1)
    pass_on(9, 12, 23)
    pass_on(5, 19)
    for i in range(3):
        pass_on(10 + i, 24 + i)
    for j in (13, 14, 15, 16, 17, 18, 19, 20, 21, 22, 23, 24, 25, 26):
        for w in range(2):
            jobs[w, j].wait_recv()
    for w in range(2):
        for j in range(27):
            jobs[w, j].wait_send()
        keep[w].wait()
    big.wait()


def gather_attn(names, sizes, q_part, o_part, gate_part):
    group = sizes[0] * sizes[1]
    experts = gate_part.shape[0] // 2
    hbm = pl.BlockSpec(memory_space=pl.ANY)
    vmem = pl.BlockSpec(memory_space=pltpu.VMEM)
    full = lambda a: jax.ShapeDtypeStruct((group * a.shape[0], a.shape[1]), a.dtype)
    moved = 2 * group * q_part.shape[0] * (q_part.shape[1] + o_part.shape[1])
    return pl.pallas_call(
        functools.partial(gather_kernel, names, sizes), name="gather_attn",
        in_specs=[vmem, vmem, hbm], out_specs=[hbm] * 3,
        out_shape=[full(q_part), full(o_part), jax.ShapeDtypeStruct((experts,) + gate_part.shape[1:], gate_part.dtype)],
        scratch_shapes=[pltpu.SemaphoreType.DMA((2, 27)), pltpu.SemaphoreType.DMA((2, 27)), pltpu.SemaphoreType.DMA((2,)), pltpu.SemaphoreType.DMA((2,))],
        cost_estimate=pl.CostEstimate(flops=60_000_000_000, bytes_accessed=moved, transcendentals=0),
        compiler_params=pltpu.CompilerParams(has_side_effects=True),
    )(q_part, o_part, gate_part)


def qkv_kernel(rope_cols, half_dim, x_ref, gain_ref, w_ref, cos_ref, sin_ref, o_ref):
    rows_f32 = x_ref[...].astype(F32)
    inv_rms = lax.rsqrt(jnp.mean(rows_f32 * rows_f32, axis=-1, keepdims=True) + NORM_EPS)
    normed = (rows_f32 * inv_rms * gain_ref[...]).astype(BF16)
    lanes = 128
    low = lax.broadcasted_iota(jnp.int32, cos_ref.shape, 1) % (2 * half_dim) < half_dim
    for c in range(0, w_ref.shape[1], 2 * lanes):
        part = jnp.dot(normed, w_ref[:, c:c + 2 * lanes], preferred_element_type=F32).astype(BF16)
        if c >= rope_cols:
            o_ref[:, c:c + 2 * lanes] = part
            continue
        for b in range(0, 2 * lanes, lanes):
            vals = part[:, b:b + lanes].astype(F32)
            other = jnp.where(low, pltpu.roll(vals, lanes - half_dim, 1), pltpu.roll(vals, half_dim, 1))
            o_ref[:, c + b:c + b + lanes] = (vals * cos_ref[...] + other * sin_ref[...]).astype(BF16)


def qkv_project(x, gain, w_qkv, cos_t, sin_t, rope_cols, half_dim):
    toks, width = x.shape
    seq_len = cos_t.shape[0]
    cols = w_qkv.shape[1]
    fixed = lambda shape: pl.BlockSpec(shape, lambda i: (0, 0))
    return pl.pallas_call(
        functools.partial(qkv_kernel, rope_cols, half_dim), name="k_qkv", grid=(toks // seq_len,),
        in_specs=[pl.BlockSpec((seq_len, width), lambda i: (i, 0)), fixed((1, width)), fixed(w_qkv.shape), fixed(cos_t.shape), fixed(sin_t.shape)],
        out_specs=pl.BlockSpec((seq_len, cols), lambda i: (i, 0)),
        out_shape=jax.ShapeDtypeStruct((toks, cols), BF16),
        cost_estimate=pl.CostEstimate(flops=2 * toks * width * cols, bytes_accessed=2 * (toks * width + width * cols + toks * cols), transcendentals=0),
        compiler_params=pltpu.CompilerParams(vmem_limit_bytes=VMEM_LIMIT),
    )(x, gain, w_qkv, cos_t, sin_t)


def attend_kernel(group_len, head_dim, q_ref, k_ref, v_ref, *rest):
    o_ref = rest[-1]
    seq_len = q_ref.shape[0]
    tile = 256
    scale = head_dim ** -0.5 * 1.4426950408889634
    for kh in range(k_ref.shape[1] // head_dim):
        keys = k_ref[:, kh * head_dim:(kh + 1) * head_dim]
        vals = v_ref[:, kh * head_dim:(kh + 1) * head_dim]
        for g in range(group_len):
            c = (kh * group_len + g) * head_dim
            for r in range(0, seq_len, tile):
                seen = r + tile
                scores = lax.dot_general(q_ref[r:seen, c:c + head_dim], keys[:seen], (((1,), (1,)), ((), ())), preferred_element_type=F32)
                causal = lax.broadcasted_iota(jnp.int32, scores.shape, 0) + r >= lax.broadcasted_iota(jnp.int32, scores.shape, 1)
                scores = jnp.where(causal, scores, -1e30)
                top = jnp.max(scores, axis=-1, keepdims=True)
                weights = jnp.exp2((scores - top) * scale)
                probs = (weights * (1.0 / jnp.sum(weights, axis=-1, keepdims=True))).astype(BF16)
                o_ref[r:seen, c:c + head_dim] = jnp.dot(probs, vals[:seen], preferred_element_type=F32).astype(BF16)


def attend(qkv, seq, out, seq_len, num_heads, kv_heads, head_dim):
    toks = qkv.shape[0]
    group_len = num_heads // kv_heads
    pair = 128 // head_dim
    qcols = pair * group_len * head_dim
    kcol0 = num_heads * head_dim // 128
    vcol0 = (num_heads + kv_heads) * head_dim // 128
    return pl.pallas_call(
        functools.partial(attend_kernel, group_len, head_dim), grid=(kv_heads // pair,),
        in_specs=[pl.BlockSpec((seq_len, qcols), lambda j: (seq, j)), pl.BlockSpec((seq_len, 128), lambda j: (seq, kcol0 + j)),
                  pl.BlockSpec((seq_len, 128), lambda j: (seq, vcol0 + j))] + ([] if out is None else [pl.BlockSpec(memory_space=pl.ANY)]),
        out_specs=pl.BlockSpec((seq_len, qcols), lambda j: (seq, j)),
        input_output_aliases={} if out is None else {3: 0},
        out_shape=jax.ShapeDtypeStruct((toks, num_heads * head_dim), BF16),
        cost_estimate=pl.CostEstimate(flops=16 * seq_len * seq_len * num_heads * head_dim, bytes_accessed=2 * seq_len * (qkv.shape[1] + num_heads * head_dim), transcendentals=seq_len * seq_len * num_heads),
        compiler_params=pltpu.CompilerParams(vmem_limit_bytes=VMEM_LIMIT),
    )(qkv, qkv, qkv, *(() if out is None else (out,)))


def project_kernel(a_ref, w_ref, x_ref, gain_ref, h_ref, z_ref):
    proj = lax.dot_general(a_ref[...], w_ref[...], (((1,), (1,)), ((), ())), preferred_element_type=F32)
    hidden = (x_ref[...].astype(F32) + proj).astype(BF16)
    h_ref[...] = hidden
    rows_f32 = hidden.astype(F32)
    inv_rms = lax.rsqrt(jnp.mean(rows_f32 * rows_f32, axis=-1, keepdims=True) + NORM_EPS)
    z_ref[...] = (rows_f32 * inv_rms * gain_ref[...]).astype(BF16)


def project(mixed, w_out_t, x, gain):
    toks, width = x.shape
    tile = 256
    row = lambda n: pl.BlockSpec((tile, n), lambda i: (i, 0))
    fixed = lambda shape: pl.BlockSpec(shape, lambda i: (0, 0))
    return pl.pallas_call(
        project_kernel, name="k_out", grid=(toks // tile,),
        in_specs=[row(mixed.shape[1]), fixed(w_out_t.shape), row(width), fixed((1, width))],
        out_specs=[row(width)] * 2,
        out_shape=[jax.ShapeDtypeStruct((toks, width), BF16)] * 2,
        cost_estimate=pl.CostEstimate(flops=2 * toks * width * mixed.shape[1], bytes_accessed=2 * (4 * toks * width + width * width), transcendentals=0),
        compiler_params=pltpu.CompilerParams(vmem_limit_bytes=VMEM_LIMIT),
    )(mixed, w_out_t, x, gain)


def attention_block(seqs, attn_gain, w_qkv, w_out_t, num_heads, kv_heads, head_dim, moe_gain):
    num_seqs, seq_len, width = seqs.shape
    half_dim = head_dim // 2
    inv_freq = ROPE_BASE ** (-jnp.arange(half_dim, dtype=F32) * 2.0 / head_dim)
    angles = jnp.arange(seq_len, dtype=F32)[:, None] * inv_freq[None, :]
    cos_t, sin_t = jnp.cos(angles), jnp.sin(angles)
    cos_t = jnp.concatenate([cos_t] * (128 // half_dim), axis=1)
    sin_t = jnp.concatenate([-sin_t, sin_t] * (64 // half_dim), axis=1)
    x = seqs.reshape(num_seqs * seq_len, width)
    qkv = qkv_project(x, attn_gain.reshape(1, width), w_qkv, cos_t, sin_t, (num_heads + kv_heads) * head_dim, half_dim)
    mixed = None
    for seq in range(num_seqs):
        mixed = attend(qkv, seq, mixed, seq_len, num_heads, kv_heads, head_dim)
    return project(mixed, w_out_t, x, moe_gain.reshape(1, width))


def dispatch_kernel(half, cap, rank_ref, rows_ref, buf_ref, out_ref, hot_ref):
    del buf_ref
    step = pl.program_id(0)
    toks, width = rows_ref.shape
    slots = lax.broadcasted_iota(jnp.int32, (cap, toks), 0).astype(F32)
    for i in range(half):
        ranks = rank_ref[pl.ds(step * half + i, 1), :]
        hot_ref[i * cap:(i + 1) * cap, :] = jnp.where(slots == ranks, 1.0, 0.0).astype(BF16)
    for c in range(0, width, 512):
        part = jnp.dot(hot_ref[...], rows_ref[:, c:c + 512], preferred_element_type=F32)
        out_ref[:, 0, :, c:c + 512] = part.astype(BF16).reshape(half, cap, 512)


def dispatch(rank_rows, rows, buf, slot, experts, cap, sources):
    toks, width = rows.shape
    half = experts // 2
    alias = {} if buf is None else {2: 0}
    args = (rank_rows, rows) + (() if buf is None else (buf,))
    body = functools.partial(dispatch_kernel, half, cap)
    if buf is None:
        def body(rank_ref, rows_ref, out_ref, hot_ref):
            dispatch_kernel(half, cap, rank_ref, rows_ref, None, out_ref, hot_ref)
    in_specs = [pl.BlockSpec(rank_rows.shape, lambda g: (0, 0)), pl.BlockSpec((toks, width), lambda g: (0, 0))]
    if buf is not None:
        in_specs.append(pl.BlockSpec(memory_space=pl.ANY))
    return pl.pallas_call(
        body, grid=(2,),
        out_shape=jax.ShapeDtypeStruct((experts, sources, cap, width), BF16),
        in_specs=in_specs,
        out_specs=pl.BlockSpec((half, 1, cap, width), lambda g: (g, slot, 0, 0)),
        scratch_shapes=[pltpu.VMEM((half * cap, toks), BF16)],
        input_output_aliases=alias,
        cost_estimate=pl.CostEstimate(flops=2 * experts * cap * toks * width, bytes_accessed=2 * (toks + experts * cap) * width, transcendentals=0),
        compiler_params=pltpu.CompilerParams(vmem_limit_bytes=VMEM_LIMIT),
    )(*args)


def gate_up_kernel(steps, s_ref, x_ref, *refs):
    g_refs, u_refs = refs[:steps], refs[steps:2 * steps]
    m_ref, wg_ref, wu_ref = refs[2 * steps:]
    d = s_ref[1]
    depth = g_refs[0].shape[1]
    for t in range(steps):
        rows = pl.ds(pl.multiple_of(lax.rem(d + steps - t, steps) * depth, depth), depth)
        wg_ref[rows, :] = g_refs[t][0]
        wu_ref[rows, :] = u_refs[t][0]
    x = x_ref[0]
    act = jnp.dot(x, wg_ref[...], preferred_element_type=F32)
    up = jnp.dot(x, wu_ref[...], preferred_element_type=F32)
    m_ref[0] = (act * jax.nn.sigmoid(act) * up).astype(BF16)


def gate_up(scal, x, which, gates, ups):
    half, depth, ff = gates[1].shape
    steps = len(gates)
    _, rows, width = x.shape
    own = pl.BlockSpec((1, depth, ff), lambda i, s: (s[0] + i, 0, 0))
    piece = pl.BlockSpec((1, depth, ff), lambda i, s: (i, 0, 0))
    return pl.pallas_call(
        functools.partial(gate_up_kernel, steps),
        grid_spec=pltpu.PrefetchScalarGridSpec(
            num_scalar_prefetch=1, grid=(half,),
            in_specs=[pl.BlockSpec((1, rows, width), lambda i, s: (which * half + i, 0, 0))] + ([own] + [piece] * (steps - 1)) * 2,
            out_specs=pl.BlockSpec((1, rows, ff), lambda i, s: (i, 0, 0)),
            scratch_shapes=[pltpu.VMEM((width, ff), BF16)] * 2),
        out_shape=jax.ShapeDtypeStruct((half, rows, ff), BF16),
        cost_estimate=pl.CostEstimate(flops=4 * half * rows * width * ff, bytes_accessed=2 * half * (rows * width + 2 * width * ff), transcendentals=0),
        compiler_params=pltpu.CompilerParams(vmem_limit_bytes=VMEM_LIMIT),
    )(scal, x, *gates, *ups)


def combine_kernel(count, experts, halves, chunks, cuts, adds, s_ref, *refs):
    refs = list(refs)
    take = lambda n: [refs.pop(0) for _ in range(n)]
    tables, mids = take(count), [take(count) for _ in halves]
    parts = [[take(len(cuts[t])) for t in range(chunks)] for _ in halves]
    added = [take(adds) for _ in range(count)]
    outs, (w_ref,) = take(count), take(1)
    i = pl.program_id(0)
    cols = parts[0][0][0].shape[2]
    spots = [pl.ds(0, cols)] if chunks == 1 else [pl.ds(pl.multiple_of(lax.rem(s_ref[1] + chunks - t, chunks) * cols, 128), cols) for t in range(chunks)]
    plain = chunks == 1 and len(cuts[0]) == 1
    if not plain:
        for j in range(len(halves)):
            for t in range(chunks):
                for piece, (start, size) in zip(parts[j][t], cuts[t]):
                    @pl.when((i >= start) & (i < start + size))
                    def _(j=j, t=t, piece=piece):
                        w_ref[j, :, spots[t]] = piece[0]
    toks, cap = tables[0].shape[1], mids[0][0].shape[1]
    slots = lax.broadcasted_iota(jnp.int32, (toks, cap), 1).astype(F32)
    for n in range(count):
        @pl.when(i == 0)
        def _(n=n):
            if chunks > 1:
                for t in range(adds):
                    outs[n][:, spots[t]] = added[n][t][...]
            elif adds:
                outs[n][...] = added[n][0][...] if adds == 1 else added[n][0][...] + added[n][1][...]
            else:
                outs[n][...] = jnp.zeros(outs[n].shape, F32)

        table = pltpu.roll(tables[n][0], lax.rem(128 - i, 128), 1)
        total = None
        for j, h in enumerate(halves):
            e = h * (experts // 2)
            w = parts[j][0][0][0] if plain else w_ref[j]
            o = jnp.dot(mids[j][n][0], w, preferred_element_type=F32).astype(BF16)
            hot = jnp.where(slots == table[:, e:e + 1], 1.0, 0.0).astype(BF16)
            picked = jnp.dot(hot, o, preferred_element_type=F32) * table[:, experts + e:experts + e + 1]
            total = picked if total is None else total + picked
        outs[n][...] += total


def combine(scal, table, ks, groups, adds):
    sources, toks, lanes = table.shape
    half, rows, ff = groups[0][1].shape
    cap = rows // sources
    halves = [h for h, _, _ in groups]
    chunks, count = len(groups[0][2]), len(ks)
    cols = groups[0][2][0][0][0].shape[2]
    cuts = [[(start, size) for _, start, size in pieces] for pieces in groups[0][2]]
    table_spec = lambda k: pl.BlockSpec((1, toks, lanes), lambda i, s: (k, 0, 0))
    mid_spec = lambda k: pl.BlockSpec((1, cap, ff), lambda i, s: (i, k, 0))

    def piece_spec(array, start, size, h):
        if array.shape[0] > half:
            index = lambda i, s: (lax.rem(i + h * half + s[0], 2 * half), 0, 0)
        else:
            index = lambda i, s: (jnp.clip(i - start, 0, size - 1), 0, 0)
        return pl.BlockSpec((1, ff, cols), index)

    flat = [(h, p) for h, _, group in groups for pieces in group for p in pieces]
    whole = pl.BlockSpec((toks, cols * chunks), lambda i, s: (0, 0))
    single = pl.BlockSpec((toks, cols), lambda i, s: (0, 0))
    flat_adds = [a for group in adds for a in group]
    flops = count * 2 * half * len(halves) * cap * cols * chunks * (ff + toks)
    return pl.pallas_call(
        functools.partial(combine_kernel, count, 2 * half, halves, chunks, cuts, len(adds[0])),
        grid_spec=pltpu.PrefetchScalarGridSpec(
            num_scalar_prefetch=1, grid=(half,),
            in_specs=[table_spec(k) for k in ks] + [mid_spec(k) for _ in groups for k in ks] + [piece_spec(*p, h) for h, p in flat] + [single] * len(flat_adds),
            out_specs=[whole] * count,
            scratch_shapes=[pltpu.VMEM((len(halves), ff, cols * chunks), BF16)]),
        out_shape=[jax.ShapeDtypeStruct((toks, cols * chunks), F32)] * count,
        cost_estimate=pl.CostEstimate(flops=flops, bytes_accessed=2 * len(halves) * half * ff * cols * chunks + count * 8 * toks * cols * chunks, transcendentals=0),
        compiler_params=pltpu.CompilerParams(vmem_limit_bytes=VMEM_LIMIT),
    )(scal, *[table] * count, *[m for _, m, _ in groups for _ in ks], *[p[0] for _, p in flat], *flat_adds)


def finish_kernel(s_ref, h_ref, own_ref, far_ref, *refs):
    del s_ref
    refs[-1][...] = (h_ref[...].astype(F32) + (own_ref[...] + far_ref[...])).astype(BF16)


def finish(scal, hidden, own, far, out):
    toks, width = hidden.shape
    cols = far.shape[1]
    tile = toks // 2
    wide = pl.BlockSpec((tile, cols), lambda i, s: (i, s[0]))
    part = pl.BlockSpec((tile, cols), lambda i, s: (i, 0))
    return pl.pallas_call(
        finish_kernel,
        grid_spec=pltpu.PrefetchScalarGridSpec(
            num_scalar_prefetch=1, grid=(toks // tile,),
            in_specs=[wide, wide, part] + ([] if out is None else [pl.BlockSpec(memory_space=pl.ANY)]), out_specs=wide),
        out_shape=jax.ShapeDtypeStruct((toks, width), BF16),
        input_output_aliases={} if out is None else {4: 0},
        cost_estimate=pl.CostEstimate(flops=2 * toks * cols, bytes_accessed=12 * toks * cols, transcendentals=0),
        compiler_params=pltpu.CompilerParams(vmem_limit_bytes=VMEM_LIMIT),
    )(scal, hidden, own, far, *(() if out is None else (out,)))


def perm(value, axis, pairs):
    return lax.ppermute(value, axis, pairs)


def solution(mesh):
    sources = mesh.shape['expert']
    steps = mesh.shape['data']
    tok_spec = P(('rep', 'expert', 'data'), None, None)
    group_axes = ('data', 'expert')
    ring = [(i, (i + 1) % steps) for i in range(steps)]
    flip = [[(i, i ^ k) for i in range(sources)] for k in range(sources)]
    swap = [(0, 1), (1, 0)]

    def local_step(x_loc, idx_loc, gate_loc, attn_gain, qkv_part, out_part, moe_gain, gate_part, up_part, down_part):
        rep, data, expert = (lax.axis_index(a) for a in ('rep', 'data', 'expert'))
        num_seqs, seq_len, width = x_loc.shape
        toks = num_seqs * seq_len
        top_k = idx_loc.shape[-1]
        experts = gate_part.shape[0]
        half = experts // 2
        cap = 8 * ((5 * top_k * toks + 32 * experts * sources - 1) // (32 * experts * sources))
        heads_all, head_dim = qkv_part.shape[1:]
        num_heads = out_part.shape[0]

        def pieces(tag, w, mine=None):
            near, far = [], []
            for t in range(1, steps if tag != 'd' else steps - 1):
                if t > 1 or mine is None:
                    mine = perm(lax.dynamic_slice_in_dim(w, rep * half, half, 0) if mine is None else mine, 'data', ring)
                near.append(mine)
                far.append(perm(mine, 'rep', swap))
            return near, far

        w_qkv, w_out_t, g_first = gather_attn(mesh.axis_names, (steps, sources), qkv_part.reshape(qkv_part.shape[0], heads_all * head_dim),
                                              out_part.reshape(num_heads * head_dim, -1).T, gate_part)
        g_near, g_far = pieces('g', gate_part, g_first)
        u_near, u_far = pieces('u', up_part)
        d_near, d_far = pieces('d', down_part)
        whole_piece = lambda a: [(a, 0, half)]
        d_near, d_far = [whole_piece(a) for a in d_near], [whole_piece(a) for a in d_far]
        last_near, last_far = [], []
        cut = half - half // 2
        for start, stop in ((0, cut), (cut, half)):
            moved = perm(d_near[-1][0][0][start:stop], 'data', ring)
            last_near.append((moved, start, stop - start))
            last_far.append((perm(moved, 'rep', swap), start, stop - start))
        d_near, d_far = [whole_piece(down_part)] + d_near + [last_near], [whole_piece(down_part)] + d_far + [last_far]

        idx_t = idx_loc.reshape(toks, top_k).T
        gate_t = gate_loc.reshape(toks, top_k).T
        idx_all = jnp.stack([idx_t] + [lax.ppermute(idx_t, 'expert', flip[k]) for k in range(1, sources)])
        gate_all = jnp.stack([gate_t] + [lax.ppermute(gate_t, 'expert', flip[k]) for k in range(1, sources)])
        order = lax.iota(jnp.int32, experts)
        local_ids = expert * experts + (order // half + rep) % 2 * half + order % half
        match = idx_all[:, :, None, :] == local_ids[None, None, :, None]
        taken = jnp.any(match, axis=1)
        weight = jnp.sum(jnp.where(match, gate_all[:, :, None, :], 0.0), axis=1)
        before = (lax.broadcasted_iota(jnp.int32, (toks, toks), 0) < lax.broadcasted_iota(jnp.int32, (toks, toks), 1)).astype(BF16)
        rank = jnp.dot(taken.reshape(sources * experts, toks).astype(BF16), before, preferred_element_type=F32).reshape(sources, experts, toks)
        rank = jnp.where(taken & (rank < cap), rank, -1.0)
        rank_rows = jnp.pad(rank, ((0, 0), (0, 16 - experts), (0, 0)), constant_values=-1.0)
        table = jnp.pad(jnp.concatenate([rank, weight], axis=1), ((0, 0), (0, 128 - 2 * experts), (0, 0))).transpose(0, 2, 1)

        attn_gain, rank_rows, table = lax.optimization_barrier((attn_gain, rank_rows, table))
        hidden, normed = attention_block(x_loc, attn_gain, w_qkv, w_out_t, num_heads, (heads_all - num_heads) // 2, head_dim, moe_gain)
        z_y = perm(normed, 'expert', flip[2])
        z_c = perm(normed, 'expert', flip[1])
        z_yc = perm(z_y, 'expert', flip[1])
        buf = None
        for k, rows in enumerate((normed, z_c, z_y, z_yc)):
            buf = dispatch(rank_rows[k], rows, buf, k, experts, cap, sources)
        x_all = buf.reshape(experts, sources * cap, width)

        scal = jnp.stack([rep * half, data]).astype(jnp.int32)
        scal_far = jnp.stack([(1 - rep) * half, data]).astype(jnp.int32)
        mid_near = gate_up(scal, x_all, 0, [gate_part] + g_near, [up_part] + u_near)
        mid_far = gate_up(scal_far, x_all, 1, [gate_part] + g_far, [up_part] + u_far)

        near = lambda t: (0, mid_near, d_near[t:t + 1])
        beyond = lambda t: (1, mid_far, d_far[t:t + 1])
        start31, start2 = {}, {}
        for t in (0, 2, 3):
            start31[t] = combine(scal, table, (3, 1), [near(t)], [[], []])
        for t in (0, 3):
            start2[t] = list(combine(scal, table, (2,), [near(t)], [[]]))
        r1, r3, far = [], [], []
        for t in range(steps):
            if t in start31:
                p3, p1 = combine(scal, table, (3, 1), [beyond(t)], [[a] for a in start31[t]])
            else:
                p3, p1 = combine(scal, table, (3, 1), [near(t), beyond(t)], [[], []])
            r3.append(perm(p3, 'expert', flip[1]))
            r1.append(perm(p1, 'expert', flip[1]))
            groups = [beyond(t)] if t in start2 else [near(t), beyond(t)]
            a2, = combine(scal, table, (2,), groups, [start2.get(t, []) + [r3[t]]])
            far.append(perm(a2, 'expert', flip[2]))
        own, = combine(scal, table, (0,), [(0, mid_near, d_near), (1, mid_far, d_far)], [r1])
        y = None
        for t in range(steps):
            y = finish(((data + steps - t) % steps).reshape(1).astype(jnp.int32), hidden, own, far[t], y)
        return y.reshape(num_seqs, seq_len, width)

    in_specs = (tok_spec, tok_spec, tok_spec, P(None), P(group_axes, None, None), P(None, None, group_axes), P(None), P('expert', 'data', None), P('expert', 'data', None), P('expert', None, 'data'))

    return jax.shard_map(local_step, mesh=mesh, in_specs=in_specs, out_specs=tok_spec, check_vma=False)
```

```python
import functools

import jax
import jax.numpy as jnp
from jax import lax
from jax.experimental import pallas as pl
from jax.experimental.pallas import tpu as pltpu
from jax.sharding import PartitionSpec as P


NORM_EPS = 1e-6
ROPE_BASE = 10000.0
F32 = jnp.float32
BF16 = jnp.bfloat16
VMEM_LIMIT = 58 * 1024 * 1024


def gather_kernel(names, sizes, q_ref, o_ref, g_ref, wq_ref, wo_ref, g1_ref, send, recv, extra, local):
    rep, data, expert = (lax.axis_index(n) for n in names)
    steps, sources = sizes
    after = lax.rem(data + 1, steps)
    across = lax.rem(expert + 2, sources)
    mate = expert + 1 - 2 * lax.rem(expert, 2)
    pairs = ((q_ref, wq_ref), (o_ref, wo_ref))
    share = q_ref.shape[0]
    half = share // 2
    right, twin, far, peer = {names[1]: after}, {names[0]: 1 - rep}, {names[2]: across}, {names[2]: mate}

    def block(w, t, e, h):
        d = lax.rem(data + steps - t, steps)
        return pairs[w][1].at[pl.ds(pl.multiple_of((d * sources + e) * share + h * half, 16), half), :]

    def whole(w, e):
        return pairs[w][1].at[pl.ds(pl.multiple_of((data * sources + e) * share, 16), share), :]

    def copy(w, j, src, dst, dev):
        return pltpu.make_async_remote_copy(src_ref=src, dst_ref=dst, send_sem=send.at[w, j], recv_sem=recv.at[w, j], device_id=dev, device_id_type=pl.DeviceIdType.MESH)

    jobs = {}
    keep = []
    for w, (own, full) in enumerate(pairs):
        mine = own.at[pl.ds(pl.multiple_of(rep * half, 16), half), :]
        keep.append(pltpu.make_async_copy(own, whole(w, expert), local.at[w]))
        jobs[w, 6] = copy(w, 6, own, whole(w, expert), far)
        jobs[w, 13] = copy(w, 13, own, whole(w, expert), peer)
        jobs[w, 20] = copy(w, 20, whole(w, across), whole(w, across), peer)
        for t in range(1, steps):
            i = t - 1
            z_src = mine if t == 1 else block(w, i, expert, rep)
            jobs[w, i] = copy(w, i, z_src, block(w, i, expert, rep), right)
            near, other = block(w, t, expert, rep), block(w, t, expert, 1 - rep)
            y_near, y_other = block(w, t, across, rep), block(w, t, across, 1 - rep)
            jobs[w, 3 + i] = copy(w, 3 + i, near, near, twin)
            jobs[w, 7 + i] = copy(w, 7 + i, near, near, far)
            jobs[w, 10 + i] = copy(w, 10 + i, y_near, y_near, twin)
            for j, b in ((14, near), (17, other), (21, y_near), (24, y_other)):
                jobs[w, j + i] = copy(w, j + i, b, b, peer)
    experts = g1_ref.shape[0]
    big = pltpu.make_async_remote_copy(src_ref=g_ref.at[pl.ds(rep * experts, experts)], dst_ref=g1_ref, send_sem=extra.at[0], recv_sem=extra.at[1],
                                       device_id=right, device_id_type=pl.DeviceIdType.MESH)

    def pass_on(arrived, *then):
        for w in range(2):
            jobs[w, arrived].wait_recv()
            for j in then:
                jobs[w, j].start()

    for w in range(2):
        for j in (0, 6, 13):
            jobs[w, j].start()
        keep[w].start()
    for i in range(3):
        pass_on(i, *(((i + 1,) if i < 2 else ()) + (3 + i, 7 + i, 14 + i)))
        if i == 2:
            big.start()
        if i == 0:
            pass_on(6, 20)
        else:
            pass_on(7 + i - 1, 10 + i - 1, 21 + i - 1)
            pass_on(3 + i - 1, 17 + i - 1)
    pass_on(9, 12, 23)
    pass_on(5, 19)
    for i in range(3):
        pass_on(10 + i, 24 + i)
    for j in (13, 14, 15, 16, 17, 18, 19, 20, 21, 22, 23, 24, 25, 26):
        for w in range(2):
            jobs[w, j].wait_recv()
    for w in range(2):
        for j in range(27):
            jobs[w, j].wait_send()
        keep[w].wait()
    big.wait()


def gather_attn(names, sizes, q_part, o_part, gate_part):
    group = sizes[0] * sizes[1]
    experts = gate_part.shape[0] // 2
    hbm = pl.BlockSpec(memory_space=pl.ANY)
    vmem = pl.BlockSpec(memory_space=pltpu.VMEM)
    full = lambda a: jax.ShapeDtypeStruct((group * a.shape[0], a.shape[1]), a.dtype)
    moved = 2 * group * q_part.shape[0] * (q_part.shape[1] + o_part.shape[1])
    return pl.pallas_call(
        functools.partial(gather_kernel, names, sizes), name="gather_attn",
        in_specs=[vmem, vmem, hbm], out_specs=[hbm] * 3,
        out_shape=[full(q_part), full(o_part), jax.ShapeDtypeStruct((experts,) + gate_part.shape[1:], gate_part.dtype)],
        scratch_shapes=[pltpu.SemaphoreType.DMA((2, 27)), pltpu.SemaphoreType.DMA((2, 27)), pltpu.SemaphoreType.DMA((2,)), pltpu.SemaphoreType.DMA((2,))],
        cost_estimate=pl.CostEstimate(flops=60_000_000_000, bytes_accessed=moved, transcendentals=0),
        compiler_params=pltpu.CompilerParams(has_side_effects=True),
    )(q_part, o_part, gate_part)


def qkv_kernel(rope_cols, half_dim, x_ref, gain_ref, w_ref, cos_ref, sin_ref, o_ref):
    rows_f32 = x_ref[...].astype(F32)
    inv_rms = lax.rsqrt(jnp.mean(rows_f32 * rows_f32, axis=-1, keepdims=True) + NORM_EPS)
    normed = (rows_f32 * inv_rms * gain_ref[...]).astype(BF16)
    lanes = 128
    low = lax.broadcasted_iota(jnp.int32, cos_ref.shape, 1) % (2 * half_dim) < half_dim
    for c in range(0, w_ref.shape[1], 2 * lanes):
        part = jnp.dot(normed, w_ref[:, c:c + 2 * lanes], preferred_element_type=F32).astype(BF16)
        if c >= rope_cols:
            o_ref[:, c:c + 2 * lanes] = part
            continue
        for b in range(0, 2 * lanes, lanes):
            vals = part[:, b:b + lanes].astype(F32)
            other = jnp.where(low, pltpu.roll(vals, lanes - half_dim, 1), pltpu.roll(vals, half_dim, 1))
            o_ref[:, c + b:c + b + lanes] = (vals * cos_ref[...] + other * sin_ref[...]).astype(BF16)


def qkv_project(x, gain, w_qkv, cos_t, sin_t, rope_cols, half_dim):
    toks, width = x.shape
    seq_len = cos_t.shape[0]
    cols = w_qkv.shape[1]
    fixed = lambda shape: pl.BlockSpec(shape, lambda i: (0, 0))
    return pl.pallas_call(
        functools.partial(qkv_kernel, rope_cols, half_dim), name="k_qkv", grid=(toks // seq_len,),
        in_specs=[pl.BlockSpec((seq_len, width), lambda i: (i, 0)), fixed((1, width)), fixed(w_qkv.shape), fixed(cos_t.shape), fixed(sin_t.shape)],
        out_specs=pl.BlockSpec((seq_len, cols), lambda i: (i, 0)),
        out_shape=jax.ShapeDtypeStruct((toks, cols), BF16),
        cost_estimate=pl.CostEstimate(flops=2 * toks * width * cols, bytes_accessed=2 * (toks * width + width * cols + toks * cols), transcendentals=0),
        compiler_params=pltpu.CompilerParams(vmem_limit_bytes=VMEM_LIMIT),
    )(x, gain, w_qkv, cos_t, sin_t)


def attend_kernel(group_len, head_dim, q_ref, k_ref, v_ref, *rest):
    o_ref = rest[-1]
    seq_len = q_ref.shape[0]
    tile = 256
    scale = head_dim ** -0.5 * 1.4426950408889634
    for kh in range(k_ref.shape[1] // head_dim):
        keys = k_ref[:, kh * head_dim:(kh + 1) * head_dim]
        vals = v_ref[:, kh * head_dim:(kh + 1) * head_dim]
        for g in range(group_len):
            c = (kh * group_len + g) * head_dim
            for r in range(0, seq_len, tile):
                seen = r + tile
                scores = lax.dot_general(q_ref[r:seen, c:c + head_dim], keys[:seen], (((1,), (1,)), ((), ())), preferred_element_type=F32)
                causal = lax.broadcasted_iota(jnp.int32, scores.shape, 0) + r >= lax.broadcasted_iota(jnp.int32, scores.shape, 1)
                scores = jnp.where(causal, scores, -1e30)
                top = jnp.max(scores, axis=-1, keepdims=True)
                weights = jnp.exp2((scores - top) * scale)
                probs = (weights * (1.0 / jnp.sum(weights, axis=-1, keepdims=True))).astype(BF16)
                o_ref[r:seen, c:c + head_dim] = jnp.dot(probs, vals[:seen], preferred_element_type=F32).astype(BF16)


def attend(qkv, seq, out, seq_len, num_heads, kv_heads, head_dim):
    toks = qkv.shape[0]
    group_len = num_heads // kv_heads
    pair = 128 // head_dim
    qcols = pair * group_len * head_dim
    kcol0 = num_heads * head_dim // 128
    vcol0 = (num_heads + kv_heads) * head_dim // 128
    return pl.pallas_call(
        functools.partial(attend_kernel, group_len, head_dim), grid=(kv_heads // pair,),
        in_specs=[pl.BlockSpec((seq_len, qcols), lambda j: (seq, j)), pl.BlockSpec((seq_len, 128), lambda j: (seq, kcol0 + j)),
                  pl.BlockSpec((seq_len, 128), lambda j: (seq, vcol0 + j))] + ([] if out is None else [pl.BlockSpec(memory_space=pl.ANY)]),
        out_specs=pl.BlockSpec((seq_len, qcols), lambda j: (seq, j)),
        input_output_aliases={} if out is None else {3: 0},
        out_shape=jax.ShapeDtypeStruct((toks, num_heads * head_dim), BF16),
        cost_estimate=pl.CostEstimate(flops=16 * seq_len * seq_len * num_heads * head_dim, bytes_accessed=2 * seq_len * (qkv.shape[1] + num_heads * head_dim), transcendentals=seq_len * seq_len * num_heads),
        compiler_params=pltpu.CompilerParams(vmem_limit_bytes=VMEM_LIMIT),
    )(qkv, qkv, qkv, *(() if out is None else (out,)))


def project_kernel(a_ref, w_ref, x_ref, gain_ref, h_ref, z_ref):
    proj = lax.dot_general(a_ref[...], w_ref[...], (((1,), (1,)), ((), ())), preferred_element_type=F32)
    hidden = (x_ref[...].astype(F32) + proj).astype(BF16)
    h_ref[...] = hidden
    rows_f32 = hidden.astype(F32)
    inv_rms = lax.rsqrt(jnp.mean(rows_f32 * rows_f32, axis=-1, keepdims=True) + NORM_EPS)
    z_ref[...] = (rows_f32 * inv_rms * gain_ref[...]).astype(BF16)


def project(mixed, w_out_t, x, gain):
    toks, width = x.shape
    tile = 256
    row = lambda n: pl.BlockSpec((tile, n), lambda i: (i, 0))
    fixed = lambda shape: pl.BlockSpec(shape, lambda i: (0, 0))
    return pl.pallas_call(
        project_kernel, name="k_out", grid=(toks // tile,),
        in_specs=[row(mixed.shape[1]), fixed(w_out_t.shape), row(width), fixed((1, width))],
        out_specs=[row(width)] * 2,
        out_shape=[jax.ShapeDtypeStruct((toks, width), BF16)] * 2,
        cost_estimate=pl.CostEstimate(flops=2 * toks * width * mixed.shape[1], bytes_accessed=2 * (4 * toks * width + width * width), transcendentals=0),
        compiler_params=pltpu.CompilerParams(vmem_limit_bytes=VMEM_LIMIT),
    )(mixed, w_out_t, x, gain)


def attention_block(seqs, attn_gain, w_qkv, w_out_t, num_heads, kv_heads, head_dim, moe_gain):
    num_seqs, seq_len, width = seqs.shape
    half_dim = head_dim // 2
    inv_freq = ROPE_BASE ** (-jnp.arange(half_dim, dtype=F32) * 2.0 / head_dim)
    angles = jnp.arange(seq_len, dtype=F32)[:, None] * inv_freq[None, :]
    cos_t, sin_t = jnp.cos(angles), jnp.sin(angles)
    cos_t = jnp.concatenate([cos_t] * (128 // half_dim), axis=1)
    sin_t = jnp.concatenate([-sin_t, sin_t] * (64 // half_dim), axis=1)
    x = seqs.reshape(num_seqs * seq_len, width)
    qkv = qkv_project(x, attn_gain.reshape(1, width), w_qkv, cos_t, sin_t, (num_heads + kv_heads) * head_dim, half_dim)
    mixed = None
    for seq in range(num_seqs):
        mixed = attend(qkv, seq, mixed, seq_len, num_heads, kv_heads, head_dim)
    return project(mixed, w_out_t, x, moe_gain.reshape(1, width))


def dispatch_kernel(half, cap, rank_ref, rows_ref, buf_ref, out_ref, hot_ref):
    del buf_ref
    step = pl.program_id(0)
    toks, width = rows_ref.shape
    slots = lax.broadcasted_iota(jnp.int32, (cap, toks), 0).astype(F32)
    for i in range(half):
        ranks = rank_ref[pl.ds(step * half + i, 1), :]
        hot_ref[i * cap:(i + 1) * cap, :] = jnp.where(slots == ranks, 1.0, 0.0).astype(BF16)
    for c in range(0, width, 512):
        part = jnp.dot(hot_ref[...], rows_ref[:, c:c + 512], preferred_element_type=F32)
        out_ref[:, 0, :, c:c + 512] = part.astype(BF16).reshape(half, cap, 512)


def dispatch(rank_rows, rows, buf, slot, experts, cap, sources):
    toks, width = rows.shape
    half = experts // 2
    alias = {} if buf is None else {2: 0}
    args = (rank_rows, rows) + (() if buf is None else (buf,))
    body = functools.partial(dispatch_kernel, half, cap)
    if buf is None:
        def body(rank_ref, rows_ref, out_ref, hot_ref):
            dispatch_kernel(half, cap, rank_ref, rows_ref, None, out_ref, hot_ref)
    in_specs = [pl.BlockSpec(rank_rows.shape, lambda g: (0, 0)), pl.BlockSpec((toks, width), lambda g: (0, 0))]
    if buf is not None:
        in_specs.append(pl.BlockSpec(memory_space=pl.ANY))
    return pl.pallas_call(
        body, grid=(2,),
        out_shape=jax.ShapeDtypeStruct((experts, sources, cap, width), BF16),
        in_specs=in_specs,
        out_specs=pl.BlockSpec((half, 1, cap, width), lambda g: (g, slot, 0, 0)),
        scratch_shapes=[pltpu.VMEM((half * cap, toks), BF16)],
        input_output_aliases=alias,
        cost_estimate=pl.CostEstimate(flops=2 * experts * cap * toks * width, bytes_accessed=2 * (toks + experts * cap) * width, transcendentals=0),
        compiler_params=pltpu.CompilerParams(vmem_limit_bytes=VMEM_LIMIT),
    )(*args)


def gate_up_kernel(steps, s_ref, x_ref, *refs):
    g_refs, u_refs = refs[:steps], refs[steps:2 * steps]
    m_ref, wg_ref, wu_ref = refs[2 * steps:]
    d = s_ref[1]
    depth = g_refs[0].shape[1]
    for t in range(steps):
        rows = pl.ds(pl.multiple_of(lax.rem(d + steps - t, steps) * depth, depth), depth)
        wg_ref[rows, :] = g_refs[t][0]
        wu_ref[rows, :] = u_refs[t][0]
    x = x_ref[0]
    act = jnp.dot(x, wg_ref[...], preferred_element_type=F32)
    up = jnp.dot(x, wu_ref[...], preferred_element_type=F32)
    m_ref[0] = (act * jax.nn.sigmoid(act) * up).astype(BF16)


def gate_up(scal, x, which, gates, ups):
    half, depth, ff = gates[1].shape
    steps = len(gates)
    _, rows, width = x.shape
    own = pl.BlockSpec((1, depth, ff), lambda i, s: (s[0] + i, 0, 0))
    piece = pl.BlockSpec((1, depth, ff), lambda i, s: (i, 0, 0))
    return pl.pallas_call(
        functools.partial(gate_up_kernel, steps),
        grid_spec=pltpu.PrefetchScalarGridSpec(
            num_scalar_prefetch=1, grid=(half,),
            in_specs=[pl.BlockSpec((1, rows, width), lambda i, s: (which * half + i, 0, 0))] + ([own] + [piece] * (steps - 1)) * 2,
            out_specs=pl.BlockSpec((1, rows, ff), lambda i, s: (i, 0, 0)),
            scratch_shapes=[pltpu.VMEM((width, ff), BF16)] * 2),
        out_shape=jax.ShapeDtypeStruct((half, rows, ff), BF16),
        cost_estimate=pl.CostEstimate(flops=4 * half * rows * width * ff, bytes_accessed=2 * half * (rows * width + 2 * width * ff), transcendentals=0),
        compiler_params=pltpu.CompilerParams(vmem_limit_bytes=VMEM_LIMIT),
    )(scal, x, *gates, *ups)


def combine_kernel(count, experts, halves, chunks, cuts, adds, s_ref, *refs):
    refs = list(refs)
    take = lambda n: [refs.pop(0) for _ in range(n)]
    tables, hots, mids = take(count), [take(count) for _ in halves], [take(count) for _ in halves]
    parts = [[take(len(cuts[t])) for t in range(chunks)] for _ in halves]
    added = [take(adds) for _ in range(count)]
    outs, (w_ref,) = take(count), take(1)
    i = pl.program_id(0)
    cols = parts[0][0][0].shape[2]
    spots = [pl.ds(0, cols)] if chunks == 1 else [pl.ds(pl.multiple_of(lax.rem(s_ref[1] + chunks - t, chunks) * cols, 128), cols) for t in range(chunks)]
    plain = chunks == 1 and len(cuts[0]) == 1
    if not plain:
        for j in range(len(halves)):
            for t in range(chunks):
                for piece, (start, size) in zip(parts[j][t], cuts[t]):
                    @pl.when((i >= start) & (i < start + size))
                    def _(j=j, t=t, piece=piece):
                        w_ref[j, :, spots[t]] = piece[0]
    pairs = [(j, n) for j in range(len(halves)) for n in range(count)]
    outcome = {}
    for j, n in pairs:
        w = parts[j][0][0][0] if plain else w_ref[j]
        outcome[j, n] = jnp.dot(mids[j][n][0], w, preferred_element_type=F32).astype(BF16)
    for n in range(count):
        @pl.when(i == 0)
        def _(n=n):
            if chunks > 1:
                for t in range(adds):
                    outs[n][:, spots[t]] = added[n][t][...]
            elif adds:
                outs[n][...] = added[n][0][...] if adds == 1 else added[n][0][...] + added[n][1][...]
            else:
                outs[n][...] = jnp.zeros(outs[n].shape, F32)
    toks = hots[0][0].shape[2]
    tile = 256
    for n in range(count):
        table = pltpu.roll(tables[n][0], lax.rem(128 - i, 128), 1)
        for r in range(0, toks, tile):
            total = None
            for j, h in enumerate(halves):
                e = experts + h * (experts // 2)
                picked = jnp.dot(hots[j][n][0, 0, r:r + tile], outcome[j, n], preferred_element_type=F32) * table[r:r + tile, e:e + 1]
                total = picked if total is None else total + picked
            outs[n][r:r + tile] += total


def select_kernel(experts, table_ref, hot_ref):
    toks, cap = hot_ref.shape[2:]
    slots = lax.broadcasted_iota(jnp.int32, (toks, cap), 1).astype(F32)
    for e in range(experts):
        hot_ref[0, e] = jnp.where(slots == table_ref[0][:, e:e + 1], 1.0, 0.0).astype(BF16)


def selectors(table, experts, cap):
    sources, toks, lanes = table.shape
    return pl.pallas_call(
        functools.partial(select_kernel, experts), name="selectors", grid=(sources,),
        in_specs=[pl.BlockSpec((1, toks, lanes), lambda k: (k, 0, 0))],
        out_specs=pl.BlockSpec((1, experts, toks, cap), lambda k: (k, 0, 0, 0)),
        out_shape=jax.ShapeDtypeStruct((sources, experts, toks, cap), BF16),
        cost_estimate=pl.CostEstimate(flops=4_000_000_000, bytes_accessed=2 * sources * experts * toks * cap, transcendentals=0),
        compiler_params=pltpu.CompilerParams(vmem_limit_bytes=VMEM_LIMIT),
    )(table)


def combine(scal, tables, ks, groups, adds):
    table, hot = tables
    sources, toks, lanes = table.shape
    half, rows, ff = groups[0][1].shape
    cap = rows // sources
    halves = [h for h, _, _ in groups]
    chunks, count = len(groups[0][2]), len(ks)
    cols = groups[0][2][0][0][0].shape[2]
    cuts = [[(start, size) for _, start, size in pieces] for pieces in groups[0][2]]
    table_spec = lambda k: pl.BlockSpec((1, toks, lanes), lambda i, s: (k, 0, 0))
    mid_spec = lambda k: pl.BlockSpec((1, cap, ff), lambda i, s: (i, k, 0))
    hot_spec = lambda h, k: pl.BlockSpec((1, 1, toks, cap), lambda i, s: (k, h * half + i, 0, 0))

    def piece_spec(array, start, size, h):
        if array.shape[0] > half:
            index = lambda i, s: (lax.rem(i + h * half + s[0], 2 * half), 0, 0)
        else:
            index = lambda i, s: (jnp.clip(i - start, 0, size - 1), 0, 0)
        return pl.BlockSpec((1, ff, cols), index)

    flat = [(h, p) for h, _, group in groups for pieces in group for p in pieces]
    whole = pl.BlockSpec((toks, cols * chunks), lambda i, s: (0, 0))
    single = pl.BlockSpec((toks, cols), lambda i, s: (0, 0))
    flat_adds = [a for group in adds for a in group]
    flops = count * 2 * half * len(halves) * cap * cols * chunks * (ff + toks)
    return pl.pallas_call(
        functools.partial(combine_kernel, count, 2 * half, halves, chunks, cuts, len(adds[0])),
        grid_spec=pltpu.PrefetchScalarGridSpec(
            num_scalar_prefetch=1, grid=(half,),
            in_specs=[table_spec(k) for k in ks] + [hot_spec(h, k) for h in halves for k in ks] + [mid_spec(k) for _ in groups for k in ks] + [piece_spec(*p, h) for h, p in flat] + [single] * len(flat_adds),
            out_specs=[whole] * count,
            scratch_shapes=[pltpu.VMEM((len(halves), ff, cols * chunks), BF16)]),
        out_shape=[jax.ShapeDtypeStruct((toks, cols * chunks), F32)] * count,
        cost_estimate=pl.CostEstimate(flops=flops, bytes_accessed=2 * len(halves) * half * ff * cols * chunks + count * 8 * toks * cols * chunks, transcendentals=0),
        compiler_params=pltpu.CompilerParams(vmem_limit_bytes=VMEM_LIMIT),
    )(scal, *[table] * count, *[hot] * (count * len(halves)), *[m for _, m, _ in groups for _ in ks], *[p[0] for _, p in flat], *flat_adds)


def finish_kernel(s_ref, h_ref, own_ref, far_ref, *refs):
    del s_ref
    refs[-1][...] = (h_ref[...].astype(F32) + (own_ref[...] + far_ref[...])).astype(BF16)


def finish(scal, hidden, own, far, out):
    toks, width = hidden.shape
    cols = far.shape[1]
    tile = toks // 2
    wide = pl.BlockSpec((tile, cols), lambda i, s: (i, s[0]))
    part = pl.BlockSpec((tile, cols), lambda i, s: (i, 0))
    return pl.pallas_call(
        finish_kernel,
        grid_spec=pltpu.PrefetchScalarGridSpec(
            num_scalar_prefetch=1, grid=(toks // tile,),
            in_specs=[wide, wide, part] + ([] if out is None else [pl.BlockSpec(memory_space=pl.ANY)]), out_specs=wide),
        out_shape=jax.ShapeDtypeStruct((toks, width), BF16),
        input_output_aliases={} if out is None else {4: 0},
        cost_estimate=pl.CostEstimate(flops=2 * toks * cols, bytes_accessed=12 * toks * cols, transcendentals=0),
        compiler_params=pltpu.CompilerParams(vmem_limit_bytes=VMEM_LIMIT),
    )(scal, hidden, own, far, *(() if out is None else (out,)))


def perm(value, axis, pairs):
    return lax.ppermute(value, axis, pairs)


def solution(mesh):
    sources = mesh.shape['expert']
    steps = mesh.shape['data']
    tok_spec = P(('rep', 'expert', 'data'), None, None)
    group_axes = ('data', 'expert')
    ring = [(i, (i + 1) % steps) for i in range(steps)]
    flip = [[(i, i ^ k) for i in range(sources)] for k in range(sources)]
    swap = [(0, 1), (1, 0)]

    def local_step(x_loc, idx_loc, gate_loc, attn_gain, qkv_part, out_part, moe_gain, gate_part, up_part, down_part):
        rep, data, expert = (lax.axis_index(a) for a in ('rep', 'data', 'expert'))
        num_seqs, seq_len, width = x_loc.shape
        toks = num_seqs * seq_len
        top_k = idx_loc.shape[-1]
        experts = gate_part.shape[0]
        half = experts // 2
        cap = 8 * ((5 * top_k * toks + 32 * experts * sources - 1) // (32 * experts * sources))
        heads_all, head_dim = qkv_part.shape[1:]
        num_heads = out_part.shape[0]

        def pieces(tag, w, mine=None):
            near, far = [], []
            for t in range(1, steps if tag != 'd' else steps - 1):
                if t > 1 or mine is None:
                    mine = perm(lax.dynamic_slice_in_dim(w, rep * half, half, 0) if mine is None else mine, 'data', ring)
                near.append(mine)
                far.append(perm(mine, 'rep', swap))
            return near, far

        w_qkv, w_out_t, g_first = gather_attn(mesh.axis_names, (steps, sources), qkv_part.reshape(qkv_part.shape[0], heads_all * head_dim),
                                              out_part.reshape(num_heads * head_dim, -1).T, gate_part)
        g_near, g_far = pieces('g', gate_part, g_first)
        u_near, u_far = pieces('u', up_part)
        d_near, d_far = pieces('d', down_part)
        whole_piece = lambda a: [(a, 0, half)]
        d_near, d_far = [whole_piece(a) for a in d_near], [whole_piece(a) for a in d_far]
        last_near, last_far = [], []
        cut = half - half // 2
        for start, stop in ((0, cut), (cut, half)):
            moved = perm(d_near[-1][0][0][start:stop], 'data', ring)
            last_near.append((moved, start, stop - start))
            last_far.append((perm(moved, 'rep', swap), start, stop - start))
        d_near, d_far = [whole_piece(down_part)] + d_near + [last_near], [whole_piece(down_part)] + d_far + [last_far]

        idx_t = idx_loc.reshape(toks, top_k).T
        gate_t = gate_loc.reshape(toks, top_k).T
        idx_all = jnp.stack([idx_t] + [lax.ppermute(idx_t, 'expert', flip[k]) for k in range(1, sources)])
        gate_all = jnp.stack([gate_t] + [lax.ppermute(gate_t, 'expert', flip[k]) for k in range(1, sources)])
        order = lax.iota(jnp.int32, experts)
        local_ids = expert * experts + (order // half + rep) % 2 * half + order % half
        match = idx_all[:, :, None, :] == local_ids[None, None, :, None]
        taken = jnp.any(match, axis=1)
        weight = jnp.sum(jnp.where(match, gate_all[:, :, None, :], 0.0), axis=1)
        before = (lax.broadcasted_iota(jnp.int32, (toks, toks), 0) < lax.broadcasted_iota(jnp.int32, (toks, toks), 1)).astype(BF16)
        rank = jnp.dot(taken.reshape(sources * experts, toks).astype(BF16), before, preferred_element_type=F32).reshape(sources, experts, toks)
        rank = jnp.where(taken & (rank < cap), rank, -1.0)
        rank_rows = jnp.pad(rank, ((0, 0), (0, 16 - experts), (0, 0)), constant_values=-1.0)
        table = jnp.pad(jnp.concatenate([rank, weight], axis=1), ((0, 0), (0, 128 - 2 * experts), (0, 0))).transpose(0, 2, 1)

        attn_gain, rank_rows, table = lax.optimization_barrier((attn_gain, rank_rows, table))
        hidden, normed = attention_block(x_loc, attn_gain, w_qkv, w_out_t, num_heads, (heads_all - num_heads) // 2, head_dim, moe_gain)
        z_y = perm(normed, 'expert', flip[2])
        z_c = perm(normed, 'expert', flip[1])
        z_yc = perm(z_y, 'expert', flip[1])
        buf = None
        for k, rows in enumerate((normed, z_c, z_y, z_yc)):
            buf = dispatch(rank_rows[k], rows, buf, k, experts, cap, sources)
        x_all = buf.reshape(experts, sources * cap, width)

        scal = jnp.stack([rep * half, data]).astype(jnp.int32)
        scal_far = jnp.stack([(1 - rep) * half, data]).astype(jnp.int32)
        mid_near = gate_up(scal, x_all, 0, [gate_part] + g_near, [up_part] + u_near)
        mid_far = gate_up(scal_far, x_all, 1, [gate_part] + g_far, [up_part] + u_far)

        table = (table, selectors(table, experts, cap))
        near = lambda t: (0, mid_near, d_near[t:t + 1])
        beyond = lambda t: (1, mid_far, d_far[t:t + 1])
        start31, start2 = {}, {}
        for t, ks in ((0, (3, 1, 2)), (2, (3, 1)), (3, (3, 1))):
            sums = list(combine(scal, table, ks, [near(t)], [[]] * len(ks)))
            start31[t] = sums[:2]
            if sums[2:]:
                start2[t] = sums[2:]
        start2[3] = list(combine(scal, table, (2,), [near(3)], [[]]))
        r1, r3, far = [], [], []
        for t in range(steps):
            if t in start31:
                p3, p1 = combine(scal, table, (3, 1), [beyond(t)], [[a] for a in start31[t]])
            else:
                p3, p1 = combine(scal, table, (3, 1), [near(t), beyond(t)], [[], []])
            r3.append(perm(p3, 'expert', flip[1]))
            r1.append(perm(p1, 'expert', flip[1]))
            groups = [beyond(t)] if t in start2 else [near(t), beyond(t)]
            a2, = combine(scal, table, (2,), groups, [start2.get(t, []) + [r3[t]]])
            far.append(perm(a2, 'expert', flip[2]))
        own, = combine(scal, table, (0,), [(0, mid_near, d_near), (1, mid_far, d_far)], [r1])
        y = None
        for t in range(steps):
            y = finish(((data + steps - t) % steps).reshape(1).astype(jnp.int32), hidden, own, far[t], y)
        return y.reshape(num_seqs, seq_len, width)

    in_specs = (tok_spec, tok_spec, tok_spec, P(None), P(group_axes, None, None), P(None, None, group_axes), P(None), P('expert', 'data', None), P('expert', 'data', None), P('expert', None, 'data'))

    return jax.shard_map(local_step, mesh=mesh, in_specs=in_specs, out_specs=tok_spec, check_vma=False)
```

```python
import functools

import jax
import jax.numpy as jnp
from jax import lax
from jax.experimental import pallas as pl
from jax.experimental.pallas import tpu as pltpu
from jax.sharding import PartitionSpec as P


NORM_EPS = 1e-6
ROPE_BASE = 10000.0
F32 = jnp.float32
BF16 = jnp.bfloat16
VMEM_LIMIT = 58 * 1024 * 1024


def gather_kernel(names, sizes, q_ref, o_ref, g_ref, wq_ref, wo_ref, g1_ref, send, recv, extra, local):
    rep, data, expert = (lax.axis_index(n) for n in names)
    steps, sources = sizes
    after = lax.rem(data + 1, steps)
    across = lax.rem(expert + 2, sources)
    mate = expert + 1 - 2 * lax.rem(expert, 2)
    pairs = ((q_ref, wq_ref), (o_ref, wo_ref))
    share = q_ref.shape[0]
    half = share // 2
    right, twin, far, peer = {names[1]: after}, {names[0]: 1 - rep}, {names[2]: across}, {names[2]: mate}

    def block(w, t, e, h):
        d = lax.rem(data + steps - t, steps)
        return pairs[w][1].at[pl.ds(pl.multiple_of((d * sources + e) * share + h * half, 16), half), :]

    def whole(w, e):
        return pairs[w][1].at[pl.ds(pl.multiple_of((data * sources + e) * share, 16), share), :]

    def copy(w, j, src, dst, dev):
        return pltpu.make_async_remote_copy(src_ref=src, dst_ref=dst, send_sem=send.at[w, j], recv_sem=recv.at[w, j], device_id=dev, device_id_type=pl.DeviceIdType.MESH)

    jobs = {}
    keep = []
    for w, (own, full) in enumerate(pairs):
        mine = own.at[pl.ds(pl.multiple_of(rep * half, 16), half), :]
        keep.append(pltpu.make_async_copy(own, whole(w, expert), local.at[w]))
        jobs[w, 6] = copy(w, 6, own, whole(w, expert), far)
        jobs[w, 13] = copy(w, 13, own, whole(w, expert), peer)
        jobs[w, 20] = copy(w, 20, whole(w, across), whole(w, across), peer)
        for t in range(1, steps):
            i = t - 1
            z_src = mine if t == 1 else block(w, i, expert, rep)
            jobs[w, i] = copy(w, i, z_src, block(w, i, expert, rep), right)
            near, other = block(w, t, expert, rep), block(w, t, expert, 1 - rep)
            y_near, y_other = block(w, t, across, rep), block(w, t, across, 1 - rep)
            jobs[w, 3 + i] = copy(w, 3 + i, near, near, twin)
            jobs[w, 7 + i] = copy(w, 7 + i, near, near, far)
            jobs[w, 10 + i] = copy(w, 10 + i, y_near, y_near, twin)
            for j, b in ((14, near), (17, other), (21, y_near), (24, y_other)):
                jobs[w, j + i] = copy(w, j + i, b, b, peer)
    experts = g1_ref.shape[0]
    big = pltpu.make_async_remote_copy(src_ref=g_ref.at[pl.ds(rep * experts, experts)], dst_ref=g1_ref, send_sem=extra.at[0], recv_sem=extra.at[1],
                                       device_id=right, device_id_type=pl.DeviceIdType.MESH)

    def pass_on(arrived, *then):
        for w in range(2):
            jobs[w, arrived].wait_recv()
            for j in then:
                jobs[w, j].start()

    for w in range(2):
        for j in (0, 6, 13):
            jobs[w, j].start()
        keep[w].start()
    for i in range(3):
        pass_on(i, *(((i + 1,) if i < 2 else ()) + (3 + i, 7 + i, 14 + i)))
        if i == 2:
            big.start()
        if i == 0:
            pass_on(6, 20)
        else:
            pass_on(7 + i - 1, 10 + i - 1, 21 + i - 1)
            pass_on(3 + i - 1, 17 + i - 1)
    pass_on(9, 12, 23)
    pass_on(5, 19)
    for i in range(3):
        pass_on(10 + i, 24 + i)
    for j in (13, 14, 15, 16, 17, 18, 19, 20, 21, 22, 23, 24, 25, 26):
        for w in range(2):
            jobs[w, j].wait_recv()
    for w in range(2):
        for j in range(27):
            jobs[w, j].wait_send()
        keep[w].wait()
    big.wait()


def gather_attn(names, sizes, q_part, o_part, gate_part):
    group = sizes[0] * sizes[1]
    experts = gate_part.shape[0] // 2
    hbm = pl.BlockSpec(memory_space=pl.ANY)
    vmem = pl.BlockSpec(memory_space=pltpu.VMEM)
    full = lambda a: jax.ShapeDtypeStruct((group * a.shape[0], a.shape[1]), a.dtype)
    moved = 2 * group * q_part.shape[0] * (q_part.shape[1] + o_part.shape[1])
    return pl.pallas_call(
        functools.partial(gather_kernel, names, sizes), name="gather_attn",
        in_specs=[vmem, vmem, hbm], out_specs=[hbm] * 3,
        out_shape=[full(q_part), full(o_part), jax.ShapeDtypeStruct((experts,) + gate_part.shape[1:], gate_part.dtype)],
        scratch_shapes=[pltpu.SemaphoreType.DMA((2, 27)), pltpu.SemaphoreType.DMA((2, 27)), pltpu.SemaphoreType.DMA((2,)), pltpu.SemaphoreType.DMA((2,))],
        cost_estimate=pl.CostEstimate(flops=60_000_000_000, bytes_accessed=moved, transcendentals=0),
        compiler_params=pltpu.CompilerParams(has_side_effects=True),
    )(q_part, o_part, gate_part)


def qkv_kernel(rope_cols, half_dim, x_ref, gain_ref, w_ref, cos_ref, sin_ref, o_ref):
    rows_f32 = x_ref[...].astype(F32)
    inv_rms = lax.rsqrt(jnp.mean(rows_f32 * rows_f32, axis=-1, keepdims=True) + NORM_EPS)
    normed = (rows_f32 * inv_rms * gain_ref[...]).astype(BF16)
    lanes = 128
    low = lax.broadcasted_iota(jnp.int32, cos_ref.shape, 1) % (2 * half_dim) < half_dim
    for c in range(0, w_ref.shape[1], 2 * lanes):
        part = jnp.dot(normed, w_ref[:, c:c + 2 * lanes], preferred_element_type=F32).astype(BF16)
        if c >= rope_cols:
            o_ref[:, c:c + 2 * lanes] = part
            continue
        for b in range(0, 2 * lanes, lanes):
            vals = part[:, b:b + lanes].astype(F32)
            other = jnp.where(low, pltpu.roll(vals, lanes - half_dim, 1), pltpu.roll(vals, half_dim, 1))
            o_ref[:, c + b:c + b + lanes] = (vals * cos_ref[...] + other * sin_ref[...]).astype(BF16)


def qkv_project(x, gain, w_qkv, cos_t, sin_t, rope_cols, half_dim):
    toks, width = x.shape
    seq_len = cos_t.shape[0]
    cols = w_qkv.shape[1]
    fixed = lambda shape: pl.BlockSpec(shape, lambda i: (0, 0))
    return pl.pallas_call(
        functools.partial(qkv_kernel, rope_cols, half_dim), name="k_qkv", grid=(toks // seq_len,),
        in_specs=[pl.BlockSpec((seq_len, width), lambda i: (i, 0)), fixed((1, width)), fixed(w_qkv.shape), fixed(cos_t.shape), fixed(sin_t.shape)],
        out_specs=pl.BlockSpec((seq_len, cols), lambda i: (i, 0)),
        out_shape=jax.ShapeDtypeStruct((toks, cols), BF16),
        cost_estimate=pl.CostEstimate(flops=2 * toks * width * cols, bytes_accessed=2 * (toks * width + width * cols + toks * cols), transcendentals=0),
        compiler_params=pltpu.CompilerParams(vmem_limit_bytes=VMEM_LIMIT),
    )(x, gain, w_qkv, cos_t, sin_t)


def attend_kernel(group_len, head_dim, q_ref, k_ref, v_ref, *rest):
    o_ref = rest[-1]
    seq_len = q_ref.shape[0]
    tile = 256
    scale = head_dim ** -0.5 * 1.4426950408889634
    for kh in range(k_ref.shape[1] // head_dim):
        keys = k_ref[:, kh * head_dim:(kh + 1) * head_dim]
        vals = v_ref[:, kh * head_dim:(kh + 1) * head_dim]
        for g in range(group_len):
            c = (kh * group_len + g) * head_dim
            for r in range(0, seq_len, tile):
                seen = r + tile
                scores = lax.dot_general(q_ref[r:seen, c:c + head_dim], keys[:seen], (((1,), (1,)), ((), ())), preferred_element_type=F32)
                causal = lax.broadcasted_iota(jnp.int32, scores.shape, 0) + r >= lax.broadcasted_iota(jnp.int32, scores.shape, 1)
                scores = jnp.where(causal, scores, -1e30)
                top = jnp.max(scores, axis=-1, keepdims=True)
                weights = jnp.exp2((scores - top) * scale)
                probs = (weights * (1.0 / jnp.sum(weights, axis=-1, keepdims=True))).astype(BF16)
                o_ref[r:seen, c:c + head_dim] = jnp.dot(probs, vals[:seen], preferred_element_type=F32).astype(BF16)


def attend(qkv, seq, out, seq_len, num_heads, kv_heads, head_dim):
    toks = qkv.shape[0]
    group_len = num_heads // kv_heads
    pair = 128 // head_dim
    qcols = pair * group_len * head_dim
    kcol0 = num_heads * head_dim // 128
    vcol0 = (num_heads + kv_heads) * head_dim // 128
    return pl.pallas_call(
        functools.partial(attend_kernel, group_len, head_dim), grid=(kv_heads // pair,),
        in_specs=[pl.BlockSpec((seq_len, qcols), lambda j: (seq, j)), pl.BlockSpec((seq_len, 128), lambda j: (seq, kcol0 + j)),
                  pl.BlockSpec((seq_len, 128), lambda j: (seq, vcol0 + j))] + ([] if out is None else [pl.BlockSpec(memory_space=pl.ANY)]),
        out_specs=pl.BlockSpec((seq_len, qcols), lambda j: (seq, j)),
        input_output_aliases={} if out is None else {3: 0},
        out_shape=jax.ShapeDtypeStruct((toks, num_heads * head_dim), BF16),
        cost_estimate=pl.CostEstimate(flops=16 * seq_len * seq_len * num_heads * head_dim, bytes_accessed=2 * seq_len * (qkv.shape[1] + num_heads * head_dim), transcendentals=seq_len * seq_len * num_heads),
        compiler_params=pltpu.CompilerParams(vmem_limit_bytes=VMEM_LIMIT),
    )(qkv, qkv, qkv, *(() if out is None else (out,)))


def project_kernel(a_ref, w_ref, x_ref, gain_ref, h_ref, z_ref):
    proj = lax.dot_general(a_ref[...], w_ref[...], (((1,), (1,)), ((), ())), preferred_element_type=F32)
    hidden = (x_ref[...].astype(F32) + proj).astype(BF16)
    h_ref[...] = hidden
    rows_f32 = hidden.astype(F32)
    inv_rms = lax.rsqrt(jnp.mean(rows_f32 * rows_f32, axis=-1, keepdims=True) + NORM_EPS)
    z_ref[...] = (rows_f32 * inv_rms * gain_ref[...]).astype(BF16)


def project(mixed, w_out_t, x, gain):
    toks, width = x.shape
    tile = 256
    row = lambda n: pl.BlockSpec((tile, n), lambda i: (i, 0))
    fixed = lambda shape: pl.BlockSpec(shape, lambda i: (0, 0))
    return pl.pallas_call(
        project_kernel, name="k_out", grid=(toks // tile,),
        in_specs=[row(mixed.shape[1]), fixed(w_out_t.shape), row(width), fixed((1, width))],
        out_specs=[row(width)] * 2,
        out_shape=[jax.ShapeDtypeStruct((toks, width), BF16)] * 2,
        cost_estimate=pl.CostEstimate(flops=2 * toks * width * mixed.shape[1], bytes_accessed=2 * (4 * toks * width + width * width), transcendentals=0),
        compiler_params=pltpu.CompilerParams(vmem_limit_bytes=VMEM_LIMIT),
    )(mixed, w_out_t, x, gain)


def attention_block(seqs, attn_gain, w_qkv, w_out_t, num_heads, kv_heads, head_dim, moe_gain):
    num_seqs, seq_len, width = seqs.shape
    half_dim = head_dim // 2
    inv_freq = ROPE_BASE ** (-jnp.arange(half_dim, dtype=F32) * 2.0 / head_dim)
    angles = jnp.arange(seq_len, dtype=F32)[:, None] * inv_freq[None, :]
    cos_t, sin_t = jnp.cos(angles), jnp.sin(angles)
    cos_t = jnp.concatenate([cos_t] * (128 // half_dim), axis=1)
    sin_t = jnp.concatenate([-sin_t, sin_t] * (64 // half_dim), axis=1)
    x = seqs.reshape(num_seqs * seq_len, width)
    qkv = qkv_project(x, attn_gain.reshape(1, width), w_qkv, cos_t, sin_t, (num_heads + kv_heads) * head_dim, half_dim)
    mixed = None
    for seq in range(num_seqs):
        mixed = attend(qkv, seq, mixed, seq_len, num_heads, kv_heads, head_dim)
    return project(mixed, w_out_t, x, moe_gain.reshape(1, width))


def dispatch_kernel(half, cap, rank_ref, rows_ref, buf_ref, out_ref, hot_ref):
    del buf_ref
    step = pl.program_id(0)
    toks, width = rows_ref.shape
    slots = lax.broadcasted_iota(jnp.int32, (cap, toks), 0).astype(F32)
    for i in range(half):
        ranks = rank_ref[pl.ds(step * half + i, 1), :]
        hot_ref[i * cap:(i + 1) * cap, :] = jnp.where(slots == ranks, 1.0, 0.0).astype(BF16)
    for c in range(0, width, 512):
        part = jnp.dot(hot_ref[...], rows_ref[:, c:c + 512], preferred_element_type=F32)
        out_ref[:, 0, :, c:c + 512] = part.astype(BF16).reshape(half, cap, 512)


def dispatch(rank_rows, rows, buf, slot, experts, cap, sources):
    toks, width = rows.shape
    half = experts // 2
    alias = {} if buf is None else {2: 0}
    args = (rank_rows, rows) + (() if buf is None else (buf,))
    body = functools.partial(dispatch_kernel, half, cap)
    if buf is None:
        def body(rank_ref, rows_ref, out_ref, hot_ref):
            dispatch_kernel(half, cap, rank_ref, rows_ref, None, out_ref, hot_ref)
    in_specs = [pl.BlockSpec(rank_rows.shape, lambda g: (0, 0)), pl.BlockSpec((toks, width), lambda g: (0, 0))]
    if buf is not None:
        in_specs.append(pl.BlockSpec(memory_space=pl.ANY))
    return pl.pallas_call(
        body, grid=(2,),
        out_shape=jax.ShapeDtypeStruct((experts, sources, cap, width), BF16),
        in_specs=in_specs,
        out_specs=pl.BlockSpec((half, 1, cap, width), lambda g: (g, slot, 0, 0)),
        scratch_shapes=[pltpu.VMEM((half * cap, toks), BF16)],
        input_output_aliases=alias,
        cost_estimate=pl.CostEstimate(flops=2 * experts * cap * toks * width, bytes_accessed=2 * (toks + experts * cap) * width, transcendentals=0),
        compiler_params=pltpu.CompilerParams(vmem_limit_bytes=VMEM_LIMIT),
    )(*args)


def gate_up_kernel(steps, s_ref, x_ref, *refs):
    g_refs, u_refs = refs[:steps], refs[steps:2 * steps]
    m_ref, wg_ref, wu_ref = refs[2 * steps:]
    d = s_ref[1]
    depth = g_refs[0].shape[1]
    for t in range(steps):
        rows = pl.ds(pl.multiple_of(lax.rem(d + steps - t, steps) * depth, depth), depth)
        wg_ref[rows, :] = g_refs[t][0]
        wu_ref[rows, :] = u_refs[t][0]
    x = x_ref[0]
    act = jnp.dot(x, wg_ref[...], preferred_element_type=F32)
    up = jnp.dot(x, wu_ref[...], preferred_element_type=F32)
    m_ref[0] = (act * jax.nn.sigmoid(act) * up).astype(BF16)


def gate_up(scal, x, which, gates, ups):
    half, depth, ff = gates[1].shape
    steps = len(gates)
    _, rows, width = x.shape
    own = pl.BlockSpec((1, depth, ff), lambda i, s: (s[0] + i, 0, 0))
    piece = pl.BlockSpec((1, depth, ff), lambda i, s: (i, 0, 0))
    return pl.pallas_call(
        functools.partial(gate_up_kernel, steps),
        grid_spec=pltpu.PrefetchScalarGridSpec(
            num_scalar_prefetch=1, grid=(half,),
            in_specs=[pl.BlockSpec((1, rows, width), lambda i, s: (which * half + i, 0, 0))] + ([own] + [piece] * (steps - 1)) * 2,
            out_specs=pl.BlockSpec((1, rows, ff), lambda i, s: (i, 0, 0)),
            scratch_shapes=[pltpu.VMEM((width, ff), BF16)] * 2),
        out_shape=jax.ShapeDtypeStruct((half, rows, ff), BF16),
        cost_estimate=pl.CostEstimate(flops=4 * half * rows * width * ff, bytes_accessed=2 * half * (rows * width + 2 * width * ff), transcendentals=0),
        compiler_params=pltpu.CompilerParams(vmem_limit_bytes=VMEM_LIMIT),
    )(scal, x, *gates, *ups)


def combine_kernel(count, experts, halves, chunks, cuts, adds, s_ref, *refs):
    refs = list(refs)
    take = lambda n: [refs.pop(0) for _ in range(n)]
    tables, mids = take(count), [take(count) for _ in halves]
    parts = [[take(len(cuts[t])) for t in range(chunks)] for _ in halves]
    added = [take(adds) for _ in range(count)]
    outs, (w_ref,) = take(count), take(1)
    i = pl.program_id(0)
    cols = parts[0][0][0].shape[2]
    spots = [pl.ds(0, cols)] if chunks == 1 else [pl.ds(pl.multiple_of(lax.rem(s_ref[1] + chunks - t, chunks) * cols, 128), cols) for t in range(chunks)]
    plain = chunks == 1 and len(cuts[0]) == 1
    if not plain:
        for j in range(len(halves)):
            for t in range(chunks):
                for piece, (start, size) in zip(parts[j][t], cuts[t]):
                    @pl.when((i >= start) & (i < start + size))
                    def _(j=j, t=t, piece=piece):
                        w_ref[j, :, spots[t]] = piece[0]
    toks, cap = tables[0].shape[1], mids[0][0].shape[1]
    slots = lax.broadcasted_iota(jnp.int32, (toks, cap), 1).astype(F32)
    for n in range(count):
        @pl.when(i == 0)
        def _(n=n):
            if chunks > 1:
                for t in range(adds):
                    outs[n][:, spots[t]] = added[n][t][...]
            elif adds:
                outs[n][...] = added[n][0][...] if adds == 1 else added[n][0][...] + added[n][1][...]
            else:
                outs[n][...] = jnp.zeros(outs[n].shape, F32)

        table = pltpu.roll(tables[n][0], lax.rem(128 - i, 128), 1)
        total = None
        for j, h in enumerate(halves):
            e = h * (experts // 2)
            w = parts[j][0][0][0] if plain else w_ref[j]
            o = jnp.dot(mids[j][n][0], w, preferred_element_type=F32).astype(BF16)
            hot = jnp.where(slots == table[:, e:e + 1], 1.0, 0.0).astype(BF16)
            picked = jnp.dot(hot, o, preferred_element_type=F32) * table[:, experts + e:experts + e + 1]
            total = picked if total is None else total + picked
        outs[n][...] += total


def combine(scal, table, ks, groups, adds):
    sources, toks, lanes = table.shape
    half, rows, ff = groups[0][1].shape
    cap = rows // sources
    halves = [h for h, _, _ in groups]
    chunks, count = len(groups[0][2]), len(ks)
    cols = groups[0][2][0][0][0].shape[2]
    cuts = [[(start, size) for _, start, size in pieces] for pieces in groups[0][2]]
    table_spec = lambda k: pl.BlockSpec((1, toks, lanes), lambda i, s: (k, 0, 0))
    mid_spec = lambda k: pl.BlockSpec((1, cap, ff), lambda i, s: (i, k, 0))

    def piece_spec(array, start, size, h):
        if array.shape[0] > half:
            index = lambda i, s: (lax.rem(i + h * half + s[0], 2 * half), 0, 0)
        else:
            index = lambda i, s: (jnp.clip(i - start, 0, size - 1), 0, 0)
        return pl.BlockSpec((1, ff, cols), index)

    flat = [(h, p) for h, _, group in groups for pieces in group for p in pieces]
    whole = pl.BlockSpec((toks, cols * chunks), lambda i, s: (0, 0))
    single = pl.BlockSpec((toks, cols), lambda i, s: (0, 0))
    flat_adds = [a for group in adds for a in group]
    flops = count * 2 * half * len(halves) * cap * cols * chunks * (ff + toks)
    return pl.pallas_call(
        functools.partial(combine_kernel, count, 2 * half, halves, chunks, cuts, len(adds[0])),
        grid_spec=pltpu.PrefetchScalarGridSpec(
            num_scalar_prefetch=1, grid=(half,),
            in_specs=[table_spec(k) for k in ks] + [mid_spec(k) for _ in groups for k in ks] + [piece_spec(*p, h) for h, p in flat] + [single] * len(flat_adds),
            out_specs=[whole] * count,
            scratch_shapes=[pltpu.VMEM((len(halves), ff, cols * chunks), BF16)]),
        out_shape=[jax.ShapeDtypeStruct((toks, cols * chunks), F32)] * count,
        cost_estimate=pl.CostEstimate(flops=flops, bytes_accessed=2 * len(halves) * half * ff * cols * chunks + count * 8 * toks * cols * chunks, transcendentals=0),
        compiler_params=pltpu.CompilerParams(vmem_limit_bytes=VMEM_LIMIT),
    )(scal, *[table] * count, *[m for _, m, _ in groups for _ in ks], *[p[0] for _, p in flat], *flat_adds)


def finish_kernel(s_ref, h_ref, own_ref, far_ref, *refs):
    del s_ref
    refs[-1][...] = (h_ref[...].astype(F32) + (own_ref[...] + far_ref[...])).astype(BF16)


def finish(scal, hidden, own, far, out):
    toks, width = hidden.shape
    cols = far.shape[1]
    tile = toks // 2
    wide = pl.BlockSpec((tile, cols), lambda i, s: (i, s[0]))
    part = pl.BlockSpec((tile, cols), lambda i, s: (i, 0))
    return pl.pallas_call(
        finish_kernel,
        grid_spec=pltpu.PrefetchScalarGridSpec(
            num_scalar_prefetch=1, grid=(toks // tile,),
            in_specs=[wide, wide, part] + ([] if out is None else [pl.BlockSpec(memory_space=pl.ANY)]), out_specs=wide),
        out_shape=jax.ShapeDtypeStruct((toks, width), BF16),
        input_output_aliases={} if out is None else {4: 0},
        cost_estimate=pl.CostEstimate(flops=2 * toks * cols, bytes_accessed=12 * toks * cols, transcendentals=0),
        compiler_params=pltpu.CompilerParams(vmem_limit_bytes=VMEM_LIMIT),
    )(scal, hidden, own, far, *(() if out is None else (out,)))


def perm(value, axis, pairs):
    return lax.ppermute(value, axis, pairs)


def solution(mesh):
    sources = mesh.shape['expert']
    steps = mesh.shape['data']
    tok_spec = P(('rep', 'expert', 'data'), None, None)
    group_axes = ('data', 'expert')
    ring = [(i, (i + 1) % steps) for i in range(steps)]
    flip = [[(i, i ^ k) for i in range(sources)] for k in range(sources)]
    swap = [(0, 1), (1, 0)]

    def local_step(x_loc, idx_loc, gate_loc, attn_gain, qkv_part, out_part, moe_gain, gate_part, up_part, down_part):
        rep, data, expert = (lax.axis_index(a) for a in ('rep', 'data', 'expert'))
        num_seqs, seq_len, width = x_loc.shape
        toks = num_seqs * seq_len
        top_k = idx_loc.shape[-1]
        experts = gate_part.shape[0]
        half = experts // 2
        cap = 8 * ((5 * top_k * toks + 32 * experts * sources - 1) // (32 * experts * sources))
        heads_all, head_dim = qkv_part.shape[1:]
        num_heads = out_part.shape[0]

        def pieces(tag, w, mine=None):
            near, far = [], []
            for t in range(1, steps if tag != 'd' else steps - 1):
                if t > 1 or mine is None:
                    mine = perm(lax.dynamic_slice_in_dim(w, rep * half, half, 0) if mine is None else mine, 'data', ring)
                near.append(mine)
                far.append(perm(mine, 'rep', swap))
            return near, far

        w_qkv, w_out_t, g_first = gather_attn(mesh.axis_names, (steps, sources), qkv_part.reshape(qkv_part.shape[0], heads_all * head_dim),
                                              out_part.reshape(num_heads * head_dim, -1).T, gate_part)
        g_near, g_far = pieces('g', gate_part, g_first)
        u_near, u_far = pieces('u', up_part)
        d_near, d_far = pieces('d', down_part)
        whole_piece = lambda a: [(a, 0, half)]
        d_near, d_far = [whole_piece(a) for a in d_near], [whole_piece(a) for a in d_far]
        last_near, last_far = [], []
        cut = half - half // 2
        for start, stop in ((0, cut), (cut, half)):
            moved = perm(d_near[-1][0][0][start:stop], 'data', ring)
            last_near.append((moved, start, stop - start))
            last_far.append((perm(moved, 'rep', swap), start, stop - start))
        d_near, d_far = [whole_piece(down_part)] + d_near + [last_near], [whole_piece(down_part)] + d_far + [last_far]

        idx_t = idx_loc.reshape(toks, top_k).T
        gate_t = gate_loc.reshape(toks, top_k).T
        idx_all = jnp.stack([idx_t] + [lax.ppermute(idx_t, 'expert', flip[k]) for k in range(1, sources)])
        gate_all = jnp.stack([gate_t] + [lax.ppermute(gate_t, 'expert', flip[k]) for k in range(1, sources)])
        order = lax.iota(jnp.int32, experts)
        local_ids = expert * experts + (order // half + rep) % 2 * half + order % half
        match = idx_all[:, :, None, :] == local_ids[None, None, :, None]
        taken = jnp.any(match, axis=1)
        weight = jnp.sum(jnp.where(match, gate_all[:, :, None, :], 0.0), axis=1)
        before = (lax.broadcasted_iota(jnp.int32, (toks, toks), 0) < lax.broadcasted_iota(jnp.int32, (toks, toks), 1)).astype(BF16)
        rank = jnp.dot(taken.reshape(sources * experts, toks).astype(BF16), before, preferred_element_type=F32).reshape(sources, experts, toks)
        rank = jnp.where(taken & (rank < cap), rank, -1.0)
        rank_rows = jnp.pad(rank, ((0, 0), (0, 16 - experts), (0, 0)), constant_values=-1.0)
        table = jnp.pad(jnp.concatenate([rank, weight], axis=1), ((0, 0), (0, 128 - 2 * experts), (0, 0))).transpose(0, 2, 1)

        attn_gain, rank_rows, table = lax.optimization_barrier((attn_gain, rank_rows, table))
        hidden, normed = attention_block(x_loc, attn_gain, w_qkv, w_out_t, num_heads, (heads_all - num_heads) // 2, head_dim, moe_gain)
        z_y = perm(normed, 'expert', flip[2])
        z_c = perm(normed, 'expert', flip[1])
        z_yc = perm(z_y, 'expert', flip[1])
        buf = None
        for k, rows in enumerate((normed, z_c, z_y, z_yc)):
            buf = dispatch(rank_rows[k], rows, buf, k, experts, cap, sources)
        x_all = buf.reshape(experts, sources * cap, width)

        scal = jnp.stack([rep * half, data]).astype(jnp.int32)
        scal_far = jnp.stack([(1 - rep) * half, data]).astype(jnp.int32)
        mid_near = gate_up(scal, x_all, 0, [gate_part] + g_near, [up_part] + u_near)
        mid_far = gate_up(scal_far, x_all, 1, [gate_part] + g_far, [up_part] + u_far)

        near = lambda t: (0, mid_near, d_near[t:t + 1])
        beyond = lambda t: (1, mid_far, d_far[t:t + 1])
        start31, start2 = {}, {}
        for t, ks in ((0, (3, 1, 2)), (2, (3, 1)), (3, (3, 1))):
            sums = list(combine(scal, table, ks, [near(t)], [[]] * len(ks)))
            start31[t] = sums[:2]
            if sums[2:]:
                start2[t] = sums[2:]
        start2[3] = list(combine(scal, table, (2,), [near(3)], [[]]))
        r1, r3, far = [], [], []
        for t in range(steps):
            if t in start31:
                p3, p1 = combine(scal, table, (3, 1), [beyond(t)], [[a] for a in start31[t]])
            else:
                p3, p1 = combine(scal, table, (3, 1), [near(t), beyond(t)], [[], []])
            r3.append(perm(p3, 'expert', flip[1]))
            r1.append(perm(p1, 'expert', flip[1]))
            groups = [beyond(t)] if t in start2 else [near(t), beyond(t)]
            a2, = combine(scal, table, (2,), groups, [start2.get(t, []) + [r3[t]]])
            far.append(perm(a2, 'expert', flip[2]))
        own, = combine(scal, table, (0,), [(0, mid_near, d_near), (1, mid_far, d_far)], [r1])
        y = None
        for t in range(steps):
            y = finish(((data + steps - t) % steps).reshape(1).astype(jnp.int32), hidden, own, far[t], y)
        return y.reshape(num_seqs, seq_len, width)

    in_specs = (tok_spec, tok_spec, tok_spec, P(None), P(group_axes, None, None), P(None, None, group_axes), P(None), P('expert', 'data', None), P('expert', 'data', None), P('expert', None, 'data'))

    return jax.shard_map(local_step, mesh=mesh, in_specs=in_specs, out_specs=tok_spec, check_vma=False)
```
